32 devices in a mesh: depth: 16 (over z, y, x), chan: 2 (over core).
Axes of the slice: x: 2, y: 2, z: 4, core: 2. Of those that a mesh axis runs over, the one named last changes fastest.
Arguments:
- feats: bfloat16 [32, 32, 8, 128], P('chan', 'depth'), may hold values from -6 to 6
- weight_one: bfloat16 [32, 32, 27], replicated, may hold values from -0.21875 to 0.21875
- weight_two: bfloat16 [64, 32, 27], replicated, may hold values from -0.21875 to 0.21875
- cotangent: bfloat16 [64, 16, 4, 64], P('chan', 'depth'), may hold values from -6 to 6
Outputs:
- grad_feats: bfloat16 [32, 32, 8, 128], P('chan', 'depth')
- grad_weight_one: float32 [32, 32, 27], P(None, 'chan')
- grad_weight_two: float32 [64, 32, 27], P(None, 'chan')
The draws below stay inside these ranges and needn't reach their ends.
All inputs are finite; a program needn't handle non-finite values.
Results may differ from the reference program's by a relative error of at most 0.013.
Values may be sent and summed in bfloat16 or wider, within the bound.
No kernel may reach another device: no remote copies, remote signals or barrier semaphores. Data moves between devices by JAX's collectives and lax.ppermute only.
A program may use at most 128 MiB of HBM per device.

```python
import jax
import jax.numpy as jnp
from jax import lax

C0 = 32
C1 = 64
H = 8
W = 128
NZ = 32


def shard_levels(rng, dims, cuts, low, largest):
    factor_of, own = 1.0, jax.random.fold_in(rng, 6)
    for axis_at, blocks in cuts:
        draws = jnp.exp(jax.random.uniform(jax.random.fold_in(own, axis_at), (blocks,), jnp.float32, low / len(cuts), largest / len(cuts)))
        factor_of = factor_of * jnp.repeat(draws, dims[axis_at] // blocks).reshape([-1 if axis == axis_at else 1 for axis in range(len(dims))])
    return factor_of


def gaussian(rng, shape, scale, bound, cuts=(), held_as=jnp.bfloat16):
    entries = scale * jax.random.normal(rng, shape, jnp.float32)
    if cuts:
        entries = entries * shard_levels(rng, shape, cuts, -0.22, 0.18)
    return jnp.clip(entries, -bound, bound).astype(held_as)


def setup_inputs(seed: int = 0) -> dict:
    splits = jax.random.split(jax.random.key(seed), 5)
    feats = gaussian(splits[0], (C0, NZ, H, W), 1.0, 6.0, ((0, 2), (1, 16)))
    weight_one = gaussian(splits[1], (C0, C0, 27), (27 * C0) ** -0.5, 0.21875)
    weight_two = gaussian(splits[2], (C1, C0, 27), (27 * C0) ** -0.5, 0.21875)
    cotangent = gaussian(splits[3], (C1, NZ // 2, H // 2, W // 2), 1.0, 6.0, ((0, 2), (1, 16)))
    return dict(feats=feats, weight_one=weight_one, weight_two=weight_two, cotangent=cotangent)


OFFSETS = [(first, second, third) for first in range(3) for second in range(3) for third in range(3)]

def pad_all(field):
    return jnp.pad(field.astype(jnp.float32), ((0, 0), (1, 1), (1, 1), (1, 1)))

def convolve(field, weight):
    chans, planes, height, across = field.shape
    padded = pad_all(field)
    total = jnp.zeros((weight.shape[0], planes, height, across), jnp.float32)
    for index, (first, second, third) in enumerate(OFFSETS):
        window = padded[:, first:first + planes, second:second + height, third:third + across]
        total = total + jnp.einsum('oi,izhw->ozhw', weight[:, :, index].astype(jnp.float32), window, precision=lax.Precision.HIGHEST)
    return total

def transpose_conv(grads, weight):
    chans, planes, height, across = grads.shape
    padded = pad_all(grads)
    total = jnp.zeros((weight.shape[1], planes, height, across), jnp.float32)
    for index, (first, second, third) in enumerate(OFFSETS):
        window = padded[:, 2 - first:2 - first + planes, 2 - second:2 - second + height, 2 - third:2 - third + across]
        total = total + jnp.einsum('oi,ozhw->izhw', weight[:, :, index].astype(jnp.float32), window, precision=lax.Precision.HIGHEST)
    return total

def weight_grad(grads, field):
    chans, planes, height, across = field.shape
    padded = pad_all(field)
    grads_wide = grads.astype(jnp.float32)
    pieces = []
    for index, (first, second, third) in enumerate(OFFSETS):
        window = padded[:, first:first + planes, second:second + height, third:third + across]
        pieces.append(jnp.einsum('ozhw,izhw->oi', grads_wide, window, precision=lax.Precision.HIGHEST))
    return jnp.stack(pieces, axis=-1)

def slope(pre):
    sig = jax.nn.sigmoid(pre)
    return sig * (1.0 + pre * (1.0 - sig))

def one_volume(feats, weight_one, weight_two, cotangent):
    chans, planes, height, across = feats.shape
    pre_one = convolve(feats, weight_one)
    act_one = jax.nn.silu(pre_one).astype(jnp.bfloat16)
    pooled = act_one.astype(jnp.float32).reshape(chans, planes // 2, 2, height // 2, 2, across // 2, 2).mean(axis=(2, 4, 6)).astype(jnp.bfloat16)
    pre_two = convolve(pooled, weight_two)
    grad_two = (cotangent.astype(jnp.float32) * slope(pre_two)).astype(jnp.bfloat16)
    grad_weight_two = weight_grad(grad_two, pooled)
    back_pooled = transpose_conv(grad_two, weight_two)
    spread = jnp.repeat(jnp.repeat(jnp.repeat(back_pooled, 2, axis=1), 2, axis=2), 2, axis=3) * 0.125
    grad_one = (spread * slope(pre_one)).astype(jnp.bfloat16)
    grad_weight_one = weight_grad(grad_one, feats)
    grad_feats = transpose_conv(grad_one, weight_one).astype(jnp.bfloat16)
    return (grad_feats, grad_weight_one, grad_weight_two)

def reference(feats, weight_one, weight_two, cotangent):
    return one_volume(feats, weight_one, weight_two, cotangent)
```

```python
import functools

import jax
import jax.numpy as jnp
from jax import lax
from jax.experimental import pallas as pl
from jax.experimental.pallas import tpu as pltpu
from jax.sharding import PartitionSpec as P

F32 = jnp.float32
BF16 = jnp.bfloat16
BLOCK = 4
VMEM = pl.BlockSpec(memory_space=pltpu.VMEM)
SMEM = pl.BlockSpec(memory_space=pltpu.SMEM)


def log2(n):
    assert n & (n - 1) == 0
    return n.bit_length() - 1


def digits(index, *sizes):
    out = []
    for size in reversed(sizes):
        out.append(index & (size - 1))
        index = index >> log2(size)
    return out[::-1]


def iotas(rows, cols):
    return (
        lax.broadcasted_iota(jnp.int32, (rows, cols), 0),
        lax.broadcasted_iota(jnp.int32, (rows, cols), 1),
    )


def one_hot(condition, value=1.0):
    return jnp.where(condition, value, 0.0).astype(BF16)


def mm(a, b):
    return jnp.dot(a, b, preferred_element_type=F32)


def mm_t(a, b):
    return lax.dot_general(a, b, (((0,), (0,)), ((), ())), preferred_element_type=F32)


def order_matrix(chans, planes, height):
    size = chans * planes * height
    k, n = iotas(size, size)
    chan, plane, row = digits(k, chans, planes, height)
    return one_hot(n == (plane * height + row) * chans + chan)


def shifted(x):
    rows = x.shape[0]
    at = lax.broadcasted_iota(jnp.int32, x.shape, 0)
    before = jnp.where(at == 0, 0.0, pltpu.roll(x, 1, 0))
    after = jnp.where(at == rows - 1, 0.0, pltpu.roll(x, rows - 1, 0))
    return before, after


def slope_of(pre, sig):
    return sig * (1.0 + pre * (1.0 - sig))


def pack_kernel(d, feats, cot, out):
    planes, width = d.planes, d.width
    lanes = d.height * d.half
    f = mm_t(feats[...], order_matrix(d.half, planes, d.height)).astype(BF16)
    for p in range(planes):
        out[p * width : (p + 1) * width, :] = f[:, p * lanes : (p + 1) * lanes]
    c = mm_t(cot[...], order_matrix(d.half2, 1, d.height2)).astype(BF16)
    out[planes * width :, :] = c


def weight_kernel(d, w1i, w1o, w2i, w2o, f1, b1, f2, b2):
    mid, half, half2 = d.mid, d.half, d.half2
    h1, h2 = d.height, d.height2
    wide1 = h1 * mid
    own1 = h1 * half
    wide2 = h2 * 2 * half2
    k, n = iotas(mid, wide1)
    spread = mm(w1i[...], one_hot(k == (n & (mid - 1)))).astype(BF16)
    row = lax.broadcasted_iota(jnp.int32, (half, wide1), 1) >> log2(mid)
    zero = jnp.zeros((half, wide1), BF16)
    for a in range(3):
        for c in range(3):
            tiles = [spread[(9 * a + 3 * b + c) * mid : (9 * a + 3 * b + c + 1) * mid] for b in range(3)]
            for g in range(2):
                for r in range(h1):
                    strip = zero
                    for b in range(3):
                        strip = jnp.where(row == r - b + 1, tiles[b][g * half : (g + 1) * half], strip)
                    at = (g * 3 + c) * own1 + r * half
                    f1[a, at : at + half, :] = strip
    k, n = iotas(mid, own1)
    spread = mm(w1o[...], one_hot(k == (n & (half - 1)))).astype(BF16)
    row = lax.broadcasted_iota(jnp.int32, (mid, own1), 1) >> log2(half)
    zero = jnp.zeros((mid, own1), BF16)
    for a in range(3):
        for c in range(3):
            tiles = [spread[(9 * a + 3 * b + c) * mid : (9 * a + 3 * b + c + 1) * mid] for b in range(3)]
            for r in range(h1):
                strip = zero
                for b in range(3):
                    strip = jnp.where(row == r + b - 1, tiles[b], strip)
                at = (c * h1 + r) * mid
                b1[a, at : at + mid, :] = strip
    k, n = iotas(2 * half2, wide2)
    g2, r2, o2 = digits(n, 2, h2, half2)
    spread = mm(w2i[...], one_hot(k == g2 * half2 + o2)).astype(BF16)
    row = digits(lax.broadcasted_iota(jnp.int32, (half, wide2), 1), 2, h2, half2)[1]
    zero = jnp.zeros((half, wide2), BF16)
    for a in range(3):
        for c in range(3):
            tiles = [spread[(9 * a + 3 * b + c) * mid : (9 * a + 3 * b + c + 1) * mid] for b in range(3)]
            for g in range(2):
                for r in range(h2):
                    strip = zero
                    for b in range(3):
                        strip = jnp.where(row == r - b + 1, tiles[b][g * half : (g + 1) * half], strip)
                    at = ((c * 2 + g) * h2 + r) * half
                    f2[a, at : at + half, :] = strip
    k, n = iotas(mid, wide1)
    spread = mm(w2o[...], one_hot(k == (n & (mid - 1)), 0.125)).astype(BF16)
    row = lax.broadcasted_iota(jnp.int32, (half2, wide1), 1) >> (log2(mid) + 1)
    zero = jnp.zeros((half2, wide1), BF16)
    for a in range(3):
        for c in range(3):
            tiles = [
                spread[(9 * a + 3 * b + c) * 2 * half2 : (9 * a + 3 * b + c + 1) * 2 * half2] for b in range(3)
            ]
            for g in range(2):
                for r in range(h2):
                    strip = zero
                    for b in range(3):
                        strip = jnp.where(row == r + b - 1, tiles[b][g * half2 : (g + 1) * half2], strip)
                    at = ((c * 2 + g) * h2 + r) * half2
                    b2[a, at : at + half2, :] = strip


def main_kernel(
    d, scalars, lo, mi, hi, lo_x, mi_x, hi_x, f1, b1, f2, b2,
    feats_out, sums_out, xs, cs, sl, pair, zs, gs, up, g1, g1s,
):
    planes, width, wide1 = d.planes, d.width, d.height * d.mid
    width2 = width // 2
    own1 = d.height * d.half
    wide2 = d.height2 * 2 * d.half2
    own2 = d.height2 * d.half2
    zl = d.height2 * d.mid
    place, at_first, at_last = scalars[0], scalars[1], scalars[2]
    per = BLOCK * planes
    first, last = at_first > 0, at_last > 0

    def unpack(k, carry):
        at = place ^ k
        for block, pairs in enumerate(((lo, lo_x), (mi, mi_x), (hi, hi_x))):
            for g, ref in enumerate(pairs):
                for p in range(planes):
                    x = ref[k, p * width : (p + 1) * width, :]
                    before, after = shifted(x.astype(F32))
                    q = block * per + at * planes + p
                    base = g * 3 * own1
                    xs[q, :, base : base + own1] = before.astype(BF16)
                    xs[q, :, base + own1 : base + 2 * own1] = x
                    xs[q, :, base + 2 * own1 : base + 3 * own1] = after.astype(BF16)
                cs[block * BLOCK + at, :, g * own2 : (g + 1) * own2] = ref[k, planes * width :, :]
        return carry

    lax.fori_loop(0, BLOCK, unpack, 0)

    k, n = iotas(wide1, zl)
    r_in, o_in = digits(k, d.height, d.mid)
    g_in, i_in = digits(o_in, 2, d.half)
    pool = one_hot(n == (g_in * d.height2 + (r_in >> 1)) * d.half + i_in, 0.125)

    def forward(step, carry):
        q = 2 + 4 * step
        pre = jnp.zeros((4 * width, wide1), F32)
        for a in range(3):
            pre += mm(xs[pl.ds(q + a - 1, 4)].reshape(4 * width, 6 * own1), f1[a])
        sig = jax.nn.sigmoid(pre)
        sl[pl.ds(4 * step, 4)] = slope_of(pre, sig).reshape(4, width, wide1)
        act = (pre * sig).astype(BF16)
        rows = mm(act, pool).reshape(2, 2, width, zl)
        pair[...] = rows[:, 0] + rows[:, 1]
        for u in range(2):
            cell = pair[u, pl.ds(0, width2, 2), :] + pair[u, pl.ds(1, width2, 2), :]
            coarse = 1 + 2 * step + u
            outside = (first & (coarse < BLOCK)) | (last & (coarse >= 2 * BLOCK))
            cell = jnp.where(outside, 0.0, cell)
            before, after = shifted(cell)
            zs[coarse - 1, :, 0:zl] = before.astype(BF16)
            zs[coarse - 1, :, zl : 2 * zl] = cell.astype(BF16)
            zs[coarse - 1, :, 2 * zl :] = after.astype(BF16)
        return carry

    lax.fori_loop(0, (3 * per - 4) // 4, forward, 0)

    count = BLOCK + 4
    pre = jnp.zeros((count * width2, wide2), F32)
    for a in range(3):
        pre += mm(zs[a : a + count].reshape(count * width2, 3 * zl), f2[a])
    sig = jax.nn.sigmoid(pre)
    grad_two = cs[2 : 2 + count].reshape(count * width2, wide2).astype(F32) * slope_of(pre, sig)
    for u in range(count):
        g = grad_two[u * width2 : (u + 1) * width2]
        before, after = shifted(g)
        gs[u, :, 0:wide2] = after.astype(BF16)
        gs[u, :, wide2 : 2 * wide2] = g.astype(BF16)
        gs[u, :, 2 * wide2 :] = before.astype(BF16)

    inner = count - 2
    back = jnp.zeros((inner * width2, wide1), F32)
    for a in range(3):
        back += mm(gs[2 - a : 2 - a + inner].reshape(inner * width2, 3 * wide2), b2[a])
    for u in range(inner):
        b = back[u * width2 : (u + 1) * width2]
        for half in range(wide1 // 128):
            lanes = slice(half * 128, (half + 1) * 128)
            up[u * (wide1 // 128) + half, pl.ds(0, width2, 2), :] = b[:, lanes]
            up[u * (wide1 // 128) + half, pl.ds(1, width2, 2), :] = b[:, lanes]
    for u in range(2 * inner):
        q = 6 + u
        both = [up[(u // 2) * (wide1 // 128) + half] for half in range(wide1 // 128)]
        g = jnp.concatenate(both, axis=1) * sl[q - 2]
        if q < per:
            g = jnp.where(first, 0.0, g)
        if q >= 2 * per:
            g = jnp.where(last, 0.0, g)
        g1[u] = g.astype(BF16)

    for u in range(planes + 2):
        g = g1[place * planes + 1 + u]
        before, after = shifted(g.astype(F32))
        g1s[u, :, 0:wide1] = after.astype(BF16)
        g1s[u, :, wide1 : 2 * wide1] = g
        g1s[u, :, 2 * wide1 :] = before.astype(BF16)
    grad = jnp.zeros((planes * width, own1), F32)
    for a in range(3):
        grad += mm(g1s[2 - a : 2 - a + planes].reshape(planes * width, 3 * wide1), b1[a])
    grad = grad.astype(BF16)
    grad = jnp.concatenate([grad[p * width : (p + 1) * width] for p in range(planes)], axis=1)
    feats_out[...] = lax.dot_general(
        order_matrix(d.half, planes, d.height), grad, (((1,), (1,)), ((), ())), preferred_element_type=F32
    ).astype(BF16)

    def collect(parts, groups, rows, chans, lanes_used, base):
        lane = lax.broadcasted_iota(jnp.int32, (chans, 128), 1)
        for g in range(groups):
            for m in range(9):
                total = jnp.zeros((chans, 128), F32)
                for r in range(rows):
                    at = (g * rows + r) * chans
                    tile = parts[m // 3][at : at + chans, (m % 3) * 128 : (m % 3 + 1) * 128]
                    tile = pltpu.roll(tile, (64 * (m % 2) - (r - 1) * d.half) % 128, 1)
                    b = (lane & 63) >> log2(d.half)
                    if r == 0:
                        tile = jnp.where(b == 0, 0.0, tile)
                    if r == rows - 1:
                        tile = jnp.where(b == 2, 0.0, tile)
                    total += tile
                if m % 2:
                    total = jnp.where(lane < 64, held, total)
                held = total
                if m % 2 or m == 8:
                    at = base + (g * 5 + m // 2) * chans
                    sums_out[at : at + chans, :] = total.astype(BF16)

    center = g1[2 : 2 + per].reshape(per * width, wide1)
    parts = [
        mm_t(center, xs[per + a - 1 : 2 * per + a - 1, :, 0 : 3 * own1].reshape(per * width, 3 * own1))
        for a in range(3)
    ]
    collect(parts, 1, d.height, d.mid, own1, 0)
    center = gs[2 : 2 + BLOCK, :, wide2 : 2 * wide2].reshape(BLOCK * width2, wide2)
    parts = [mm_t(center, zs[2 + a : 2 + a + BLOCK].reshape(BLOCK * width2, 3 * zl)) for a in range(3)]
    collect(parts, 2, d.height2, d.half2, own2 // 2, 5 * d.mid)


def final_kernel(d, scalars, *refs):
    parts, (out1, out2, rows1, rows2) = refs[:-4], refs[-4:]
    terms = [p[...].astype(F32) for p in parts]
    while len(terms) > 1:
        terms = [terms[i] + terms[i + 1] for i in range(0, len(terms), 2)]
    total = terms[0]
    member = scalars[3]

    def lay_out(base, groups, chans, scratch, out):
        for m2 in range(5):
            tiles = [total[base + (g * 5 + m2) * chans : base + (g * 5 + m2 + 1) * chans] for g in range(groups)]
            tile = jnp.concatenate(tiles, axis=0) if groups > 1 else tiles[0]
            flat = tile.T
            for m in (2 * m2, 2 * m2 + 1):
                if m < 9:
                    for b in range(3):
                        at = 64 * (m % 2) + b * d.half
                        tap = 9 * (m // 3) + 3 * b + m % 3
                        scratch[tap * d.half : (tap + 1) * d.half, :] = flat[at : at + d.half]
        full = groups * chans
        for i in range(d.half):
            tile = scratch[pl.ds(i, 27, d.half), :]
            tile = jnp.concatenate([tile, jnp.zeros((5, full), F32)], axis=0).T
            tile = pltpu.roll(tile, member * (full // 2), 0)
            out[pl.ds(i, full, d.half), :] = tile[:, :27]

    lay_out(0, 1, d.mid, rows1, out1)
    lay_out(5 * d.mid, 2, d.half2, rows2, out2)


class Sizes:
    pass


def shards(feats, weight_one, weight_two, cotangent):
    d = Sizes()
    slabs = lax.axis_size("depth")
    groups = lax.axis_size("chan")
    assert groups == 2 and slabs % BLOCK == 0
    d.half, d.planes, d.height, d.width = feats.shape
    d.half2, coarse, d.height2, width2 = cotangent.shape
    d.mid = weight_one.shape[0]
    assert d.planes == 2 and coarse == 1 and d.half * 8 == 128 and d.height2 * d.half2 == 128
    assert d.width == 128 and d.height == 8 and d.mid == 32
    place = lax.axis_index("depth")
    member = lax.axis_index("chan")
    blocks = slabs // BLOCK
    scalars = jnp.stack(
        [
            place % BLOCK,
            (place < BLOCK).astype(jnp.int32),
            (place >= slabs - BLOCK).astype(jnp.int32),
            member,
        ]
    ).astype(jnp.int32)
    params = pltpu.CompilerParams(vmem_limit_bytes=40 * 1024 * 1024)

    rows = d.planes * d.width + width2
    item = pl.pallas_call(
        functools.partial(pack_kernel, d),
        out_shape=jax.ShapeDtypeStruct((rows, 128), BF16),
        in_specs=[VMEM] * 2,
        out_specs=VMEM,
        compiler_params=params,
        name="pack",
    )(feats.reshape(-1, d.width), cotangent.reshape(-1, width2))

    def xor(x, k):
        return lax.ppermute(x, "depth", [(i, i ^ k) for i in range(slabs)])

    def swap(x):
        return lax.ppermute(x, "chan", [(0, 1), (1, 0)])

    block = jnp.stack([item] + [xor(item, k) for k in range(1, BLOCK)])
    lo = lax.ppermute(block, "depth", [(i, i + BLOCK) for i in range(slabs - BLOCK)])
    hi = lax.ppermute(block, "depth", [(i + BLOCK, i) for i in range(slabs - BLOCK)])
    block_x, lo_x, hi_x = swap(block), swap(lo), swap(hi)

    w1 = jnp.where(member == 0, weight_one, jnp.roll(weight_one, (d.half, d.half), (0, 1)))
    w2 = jnp.where(member == 0, weight_two, jnp.roll(weight_two, (d.half2, d.half), (0, 1)))
    w1i = jnp.transpose(w1, (2, 1, 0)).reshape(27 * d.mid, d.mid)
    w1o = jnp.transpose(w1, (2, 0, 1)).reshape(27 * d.mid, d.mid)
    w2i = jnp.transpose(w2, (2, 1, 0)).reshape(27 * d.mid, 2 * d.half2)
    w2o = jnp.transpose(w2, (2, 0, 1)).reshape(27 * 2 * d.half2, d.mid)
    wide1 = d.height * d.mid
    own1 = d.height * d.half
    wide2 = d.height2 * 2 * d.half2
    zl = d.height2 * d.mid
    f1, b1, f2, b2 = pl.pallas_call(
        functools.partial(weight_kernel, d),
        out_shape=[
            jax.ShapeDtypeStruct((3, 6 * own1, wide1), BF16),
            jax.ShapeDtypeStruct((3, 3 * wide1, own1), BF16),
            jax.ShapeDtypeStruct((3, 3 * zl, wide2), BF16),
            jax.ShapeDtypeStruct((3, 3 * wide2, wide1), BF16),
        ],
        in_specs=[VMEM] * 4,
        out_specs=[VMEM] * 4,
        compiler_params=params,
        cost_estimate=pl.CostEstimate(flops=1 << 30, bytes_accessed=4 << 20, transcendentals=0),
        name="weights",
    )(w1i, w1o, w2i, w2o)

    per = BLOCK * d.planes
    grad, sums = pl.pallas_call(
        functools.partial(main_kernel, d),
        out_shape=[
            jax.ShapeDtypeStruct((d.half * d.planes * d.height, d.width), BF16),
            jax.ShapeDtypeStruct((5 * d.mid + 10 * d.half2, 128), BF16),
        ],
        in_specs=[SMEM] + [VMEM] * 10,
        out_specs=[VMEM] * 2,
        scratch_shapes=[
            pltpu.VMEM((3 * per, d.width, 6 * own1), BF16),
            pltpu.VMEM((3 * BLOCK, width2, wide2), BF16),
            pltpu.VMEM((3 * per - 4, d.width, wide1), F32),
            pltpu.VMEM((2, d.width, zl), F32),
            pltpu.VMEM((3 * BLOCK - 2, width2, 3 * zl), BF16),
            pltpu.VMEM((BLOCK + 4, width2, 3 * wide2), BF16),
            pltpu.VMEM(((BLOCK + 2) * (wide1 // 128), d.width, 128), F32),
            pltpu.VMEM((2 * (BLOCK + 2), d.width, wide1), BF16),
            pltpu.VMEM((d.planes + 2, d.width, 3 * wide1), BF16),
        ],
        compiler_params=params,
        cost_estimate=pl.CostEstimate(flops=1 << 33, bytes_accessed=8 << 20, transcendentals=0),
        name="chain",
    )(scalars, lo, block, hi, lo_x, block_x, hi_x, f1, b1, f2, b2)

    parts = [sums]
    radix = 1
    while radix < blocks:
        fan = min(4, blocks // radix)
        mine = parts[0]
        if len(parts) > 1:
            mine = sum_parts(parts)
        parts = [mine] + [xor(mine, BLOCK * radix * k) for k in range(1, fan)]
        radix *= fan
    out1, out2 = pl.pallas_call(
        functools.partial(final_kernel, d),
        out_shape=[
            jax.ShapeDtypeStruct((d.mid * d.half, 27), F32),
            jax.ShapeDtypeStruct((2 * d.half2 * d.half, 27), F32),
        ],
        in_specs=[SMEM] + [VMEM] * len(parts),
        out_specs=[VMEM] * 2,
        scratch_shapes=[
            pltpu.VMEM((27 * d.half, d.mid), F32),
            pltpu.VMEM((27 * d.half, 2 * d.half2), F32),
        ],
        compiler_params=params,
        name="finish",
    )(scalars, *parts)
    return (
        grad.reshape(feats.shape),
        out1.reshape(d.mid, d.half, 27),
        out2.reshape(2 * d.half2, d.half, 27),
    )


def sum_parts(parts):
    terms = [p.astype(F32) for p in parts]
    while len(terms) > 1:
        terms = [terms[i] + terms[i + 1] for i in range(0, len(terms), 2)]
    return terms[0].astype(BF16)


def solution(mesh):
    return jax.shard_map(
        shards,
        mesh=mesh,
        in_specs=(P("chan", "depth", None, None), P(), P(), P("chan", "depth", None, None)),
        out_specs=(P("chan", "depth", None, None), P(None, "chan", None), P(None, "chan", None)),
        check_vma=False,
    )
```

```python
import functools

import jax
import jax.numpy as jnp
from jax import lax
from jax.experimental import pallas as pl
from jax.experimental.pallas import tpu as pltpu
from jax.sharding import PartitionSpec as P

F32 = jnp.float32
BF16 = jnp.bfloat16
BLOCK = 4
EDGE = 3
VMEM = pl.BlockSpec(memory_space=pltpu.VMEM)


def log2(n):
    assert n & (n - 1) == 0
    return n.bit_length() - 1


def digits(index, *sizes):
    out = []
    for size in reversed(sizes):
        out.append(index & (size - 1))
        index = index >> log2(size)
    return out[::-1]


def iotas(rows, cols):
    return (
        lax.broadcasted_iota(jnp.int32, (rows, cols), 0),
        lax.broadcasted_iota(jnp.int32, (rows, cols), 1),
    )


def one_hot(condition, value=1.0):
    return jnp.where(condition, value, 0.0).astype(BF16)


def mm(a, b):
    return jnp.dot(a, b, preferred_element_type=F32)


def mm_t(a, b):
    return lax.dot_general(a, b, (((0,), (0,)), ((), ())), preferred_element_type=F32)


def order_matrix(chans, planes, height):
    size = chans * planes * height
    k, n = iotas(size, size)
    chan, plane, row = digits(k, chans, planes, height)
    return one_hot(n == (plane * height + row) * chans + chan)


def shifted(x):
    rows = x.shape[0]
    at = lax.broadcasted_iota(jnp.int32, x.shape, 0)
    before = jnp.where(at == 0, 0.0, pltpu.roll(x, 1, 0))
    after = jnp.where(at == rows - 1, 0.0, pltpu.roll(x, rows - 1, 0))
    return before, after


def slope_of(pre, sig):
    return sig * (1.0 + pre * (1.0 - sig))


def pack_kernel(d, feats, cot, out, feats_in, cot_in, sems):
    copies = [
        pltpu.make_async_copy(feats, feats_in, sems.at[0]),
        pltpu.make_async_copy(cot, cot_in, sems.at[1]),
    ]
    for copy in copies:
        copy.start()
    planes, width = d.planes, d.width
    lanes = d.height * d.half
    turn = order_matrix(d.half, planes, d.height)
    turn2 = order_matrix(d.half2, 1, d.height2)
    copies[0].wait()
    f = mm_t(feats_in[...], turn).astype(BF16)
    for p in range(planes):
        out[p * width : (p + 1) * width, :] = f[:, p * lanes : (p + 1) * lanes]
    copies[1].wait()
    out[planes * width :, :] = mm_t(cot_in[...], turn2).astype(BF16)


def parity():
    return (lax.axis_index("depth") >> log2(BLOCK)) & 1 == 0


def sort_kernel(d, i0, i1, i2, i3, mid, to_a, to_b):
    place = lax.axis_index("depth") & (BLOCK - 1)
    odd = (lax.axis_index("depth") >> log2(BLOCK)) & 1
    width, width2 = d.width, d.width // 2
    body = d.planes * width
    per = BLOCK * body
    for k, ref in enumerate((i0, i1, i2, i3)):
        at = place ^ k
        mid[pl.ds(at * body, body), :] = ref[:body, :]
        mid[pl.ds(per + at * width2, width2), :] = ref[body:, :]
    side = EDGE * width
    for out, top in ((to_a, 1 - odd), (to_b, odd)):
        out[:side, :] = mid[pl.ds(pl.multiple_of(top * (per - side), side // EDGE), side), :]
        out[side:, :] = mid[pl.ds(pl.multiple_of(per + top * 2 * width2, width2), 2 * width2), :]


def band(out, a, at, size, groups, row, shift):
    strip = jnp.zeros((size, row.shape[1]), BF16)
    for b in range(3):
        strip = jnp.where(row == shift[b], groups[b], strip)
    out[a, at : at + size, :] = strip


def weight_kernel(d, w1, w2, f1, b1, f2, b2, w1_in, w2_in, t1, t2, t3, t4, sems):
    copies = [pltpu.make_async_copy(w1, w1_in, sems.at[0]), pltpu.make_async_copy(w2, w2_in, sems.at[1])]
    for copy in copies:
        copy.start()
    member = lax.axis_index("chan")
    mid, half, half2 = d.mid, d.half, d.half2
    h1, h2 = d.height, d.height2
    wide1 = h1 * mid
    own1 = h1 * half
    wide2 = h2 * 2 * half2
    k, n = iotas(mid, wide1)
    own_first = (k ^ (member * half)) == (n & (mid - 1))
    for copy in copies:
        copy.wait()
    for t in range(27):
        at = slice(t * mid, (t + 1) * mid)
        t1[at, :] = mm_t(w1_in[at, :], one_hot(own_first)).astype(BF16)
        t4[t * 2 * half2 : (t + 1) * 2 * half2, :] = mm_t(w2_in[at, :], one_hot(own_first, 0.125)).astype(BF16)
    k, n = iotas(mid, own1)
    t2[...] = mm(w1_in[...], one_hot((k ^ (member * half)) == (n & (half - 1)))).astype(BF16)
    k, n = iotas(2 * half2, wide2)
    g2, _, o2 = digits(n, 2, h2, half2)
    t3[...] = mm(w2_in[...], one_hot((k ^ (member * half2)) == g2 * half2 + o2)).astype(BF16)

    def rows_of(ref, a, c, size, total, group):
        at = [(9 * a + 3 * b + c) * total + (group ^ member) * size for b in range(3)]
        return [ref[pl.ds(pl.multiple_of(x, size), size), :] for x in at]

    row1 = lax.broadcasted_iota(jnp.int32, (half, wide1), 1) >> log2(mid)
    row2 = lax.broadcasted_iota(jnp.int32, (half, own1), 1) >> log2(half)
    row3 = digits(lax.broadcasted_iota(jnp.int32, (half, wide2), 1), 2, h2, half2)[1]
    row4 = lax.broadcasted_iota(jnp.int32, (half2, wide1), 1) >> (log2(mid) + 1)
    for a in range(3):
        for c in range(3):
            for g in range(2):
                tiles = rows_of(t1, a, c, half, mid, g)
                for r in range(h1):
                    band(f1, a, (g * 3 + c) * own1 + r * half, half, tiles, row1, (r + 1, r, r - 1))
                tiles = rows_of(t2, a, c, half, mid, g)
                for r in range(h1):
                    at = (c * h1 + r) * mid + g * half
                    band(b1, a, at, half, tiles, row2, (r - 1, r, r + 1))
                tiles = rows_of(t3, a, c, half, mid, g)
                for r in range(h2):
                    at = ((c * 2 + g) * h2 + r) * half
                    band(f2, a, at, half, tiles, row3, (r + 1, r, r - 1))
                tiles = rows_of(t4, a, c, half2, 2 * half2, g)
                for r in range(h2):
                    at = ((c * 2 + g) * h2 + r) * half2
                    band(b2, a, at, half2, tiles, row4, (r - 1, r, r + 1))


def spread_plane(d, x, xs, q):
    lanes = d.height * d.half
    before, after = shifted(x.astype(F32))
    xs[q, :, 0:lanes] = before.astype(BF16)
    xs[q, :, lanes : 2 * lanes] = x
    xs[q, :, 2 * lanes :] = after.astype(BF16)


def pool_matrix(d):
    k, n = iotas(d.height * d.mid, d.height2 * d.mid)
    r, o = digits(k, d.height, d.mid)
    g, i = digits(o, 2, d.half)
    return one_hot(n == (g * d.height2 + (r >> 1)) * d.half + i, 0.125)


def half_sum(d, xs, q, count, f1, g, pre):
    size = 3 * d.height * d.half
    for a in range(3):
        pre = pre + mm(xs[q + a - 1 : q + a - 1 + count].reshape(count * d.width, size), f1[a, g * size : (g + 1) * size])
    return pre


def first_level(d, pre, count, pool, slopes, rows, at):
    sig = jax.nn.sigmoid(pre)
    slopes[at : at + count] = slope_of(pre, sig).reshape(count, d.width, -1)
    rows[at : at + count] = mm((pre * sig).astype(BF16), pool).reshape(count, d.width, -1)


def pool_pair(d, rows, at, pair, k):
    width2 = d.width // 2
    pair[k] = rows[at] + rows[at + 1]
    return pair[k, pl.ds(0, width2, 2), :] + pair[k, pl.ds(1, width2, 2), :]


def pick(lower, even, a, b, outside):
    value = jnp.where(even, b, a) if lower else jnp.where(even, a, b)
    return jnp.where(outside, jnp.zeros_like(value), value)


def ends():
    place = lax.axis_index("depth")
    return place < BLOCK, place >= lax.axis_size("depth") - BLOCK


def middle_kernel(d, mi, mi_x, f1, xs, xs_x, slopes, rows, pooled, pair):
    per = BLOCK * d.planes
    for p in range(per):
        at = slice(p * d.width, (p + 1) * d.width)
        spread_plane(d, mi[at, :], xs, EDGE + p)
        spread_plane(d, mi_x[at, :], xs_x, EDGE + p)
    pool = pool_matrix(d)
    for q in range(1, per - 1, 3):
        pre = jnp.zeros((3 * d.width, d.height * d.mid), F32)
        for g, ref in enumerate((xs, xs_x)):
            pre = half_sum(d, ref, EDGE + q, 3, f1, g, pre)
        first_level(d, pre, 3, pool, slopes, rows, q - 1)
    for u in range(BLOCK - 2):
        pooled[u] = pool_pair(d, rows, 2 * u + 1, pair, u).astype(BF16)


def outer_kernel(d, a, b, a_x, b_x, xs_in, xs_x_in, f1, xs, xs_x, slopes, rows):
    del xs_in, xs_x_in
    per = BLOCK * d.planes
    even = parity()
    first, last = ends()
    for pair, ref in (((a, b), xs), ((a_x, b_x), xs_x)):
        for p in range(EDGE):
            x, y = (r[p * d.width : (p + 1) * d.width, :] for r in pair)
            spread_plane(d, pick(True, even, x, y, first), ref, p)
            spread_plane(d, pick(False, even, x, y, last), ref, EDGE + per + p)
    pool = pool_matrix(d)
    for k, q in enumerate((1, per + EDGE - 1)):
        pre = jnp.zeros((3 * d.width, d.height * d.mid), F32)
        for g, ref in enumerate((xs, xs_x)):
            pre = half_sum(d, ref, q, 3, f1, g, pre)
        first_level(d, pre, 3, pool, slopes, rows, 3 * k)


def main_kernel(
    d, a, mi, b, a_x, mi_x, b_x, xs, slopes_mid, rows_mid, slopes_out, rows_out, pooled_a, pooled, pooled_b,
    f2, b2, grads_out, sums_out, cs, sl, rows, pair, zs, gs, up, g1,
):
    place = lax.axis_index("depth")
    first, last = ends()
    even = parity()
    planes, width, wide1 = d.planes, d.width, d.height * d.mid
    width2 = width // 2
    own1 = d.height * d.half
    wide2 = d.height2 * 2 * d.half2
    own2 = d.height2 * d.half2
    zl = d.height2 * d.mid
    per = BLOCK * planes

    side = EDGE * width
    for g, (x, m, y) in enumerate(((a, mi, b), (a_x, mi_x, b_x))):
        lanes = slice(g * own2, (g + 1) * own2)
        x, y = x[side:, :], y[side:, :]
        cs[0:2, :, lanes] = pick(True, even, x, y, first).reshape(2, width2, own2)
        cs[2 : 2 + BLOCK, :, lanes] = m[per * width :, :].reshape(BLOCK, width2, own2)
        cs[2 + BLOCK :, :, lanes] = pick(False, even, x, y, last).reshape(2, width2, own2)
    inner = per - 2
    for ref, outer, middle in ((sl, slopes_out, slopes_mid), (rows, rows_out, rows_mid)):
        ref[0:3] = outer[0:3]
        ref[3 : 3 + inner] = middle[...]
        ref[3 + inner :] = outer[3:6]
    for u in range(3 * BLOCK - 2):
        coarse = 1 + u
        if coarse < BLOCK - 1:
            k = coarse - 1
            cell = pick(True, even, pooled_a[k], pooled_b[k], first).astype(F32)
        elif coarse > 2 * BLOCK:
            k = coarse - 2 * BLOCK - 1
            cell = pick(False, even, pooled_a[k], pooled_b[k], last).astype(F32)
        elif BLOCK < coarse < 2 * BLOCK - 1:
            cell = pooled[coarse - BLOCK - 1].astype(F32)
        else:
            cell = pool_pair(d, rows, 2 * coarse - per + 2, pair, u)
        if coarse == BLOCK - 1:
            cell = jnp.where(first, 0.0, cell)
        if coarse == 2 * BLOCK:
            cell = jnp.where(last, 0.0, cell)
        before, after = shifted(cell)
        zs[u, :, 0:zl] = before.astype(BF16)
        zs[u, :, zl : 2 * zl] = cell.astype(BF16)
        zs[u, :, 2 * zl :] = after.astype(BF16)

    count = BLOCK + 4
    pre = jnp.zeros((count * width2, wide2), F32)
    for a in range(3):
        pre += mm(zs[a : a + count].reshape(count * width2, 3 * zl), f2[a])
    sig = jax.nn.sigmoid(pre)
    grad_two = cs[...].reshape(count * width2, wide2).astype(F32) * slope_of(pre, sig)
    for u in range(count):
        g = grad_two[u * width2 : (u + 1) * width2]
        before, after = shifted(g)
        gs[u, :, 0:wide2] = after.astype(BF16)
        gs[u, :, wide2 : 2 * wide2] = g.astype(BF16)
        gs[u, :, 2 * wide2 :] = before.astype(BF16)

    inner = count - 2
    back = jnp.zeros((inner * width2, wide1), F32)
    for a in range(3):
        back += mm(gs[2 - a : 2 - a + inner].reshape(inner * width2, 3 * wide2), b2[a])
    pieces = wide1 // 128
    for u in range(inner):
        b = back[u * width2 : (u + 1) * width2]
        for piece in range(pieces):
            lanes = slice(piece * 128, (piece + 1) * 128)
            up[u * pieces + piece, pl.ds(0, width2, 2), :] = b[:, lanes]
            up[u * pieces + piece, pl.ds(1, width2, 2), :] = b[:, lanes]
    for u in range(per + 2):
        q = per - 1 + u
        both = [up[(q - 6) // 2 * pieces + piece] for piece in range(pieces)]
        g = jnp.concatenate(both, axis=1) * sl[q - per + 2]
        if q < per:
            g = jnp.where(first, 0.0, g)
        if q >= 2 * per:
            g = jnp.where(last, 0.0, g)
        g1[u] = g.astype(BF16)
    grads_out[...] = g1[pl.ds((place & (BLOCK - 1)) * planes, planes + 2)]

    def collect(parts, groups, height, chans, base):
        lane = lax.broadcasted_iota(jnp.int32, (chans, 128), 1)
        tap_row = lane >> log2(d.half)
        for g in range(groups):
            def total(m):
                out = jnp.zeros((chans, 128), F32)
                for r in range(height):
                    at = (g * height + r) * chans
                    tile = parts[m // 3][at : at + chans, (m % 3) * 128 : (m % 3 + 1) * 128]
                    tile = pltpu.roll(tile, (1 - r) * d.half % 128, 1)
                    if r == 0:
                        tile = jnp.where(tap_row == 0, 0.0, tile)
                    if r == height - 1:
                        tile = jnp.where(tap_row == 2, 0.0, tile)
                    out += tile
                return out

            def turned(x, lanes):
                return pltpu.roll(x, lanes % 128, 1) if lanes % 128 else x

            extra = total(8)
            for tile in range(4):
                out = jnp.where(lane < 3 * d.half, total(2 * tile), turned(total(2 * tile + 1), 3 * d.half))
                if tile == 0:
                    out = jnp.where(lane < 6 * d.half, out, turned(extra, 6 * d.half))
                if tile == 1:
                    out = jnp.where(lane < 6 * d.half, out, turned(extra, 4 * d.half))
                at = base + (g * 4 + tile) * chans
                sums_out[at : at + chans, :] = out.astype(BF16)

    center = g1[1 : 1 + per].reshape(per * width, wide1)
    parts = [
        mm_t(center, xs[EDGE + a - 1 : EDGE + a - 1 + per].reshape(per * width, 3 * own1))
        for a in range(3)
    ]
    collect(parts, 1, d.height, d.mid, 0)
    center = gs[2 : 2 + BLOCK, :, wide2 : 2 * wide2].reshape(BLOCK * width2, wide2)
    parts = [mm_t(center, zs[2 + a : 2 + a + BLOCK].reshape(BLOCK * width2, 3 * zl)) for a in range(3)]
    collect(parts, 2, d.height2, d.half2, 4 * d.mid)


def feats_kernel(d, g1, b1, out, wide):
    planes, width, wide1 = d.planes, d.width, d.height * d.mid
    for u in range(planes + 2):
        g = g1[u]
        before, after = shifted(g.astype(F32))
        wide[u, :, 0:wide1] = after.astype(BF16)
        wide[u, :, wide1 : 2 * wide1] = g
        wide[u, :, 2 * wide1 :] = before.astype(BF16)
    grad = jnp.zeros((planes * width, d.height * d.half), F32)
    for a in range(3):
        grad += mm(wide[2 - a : 2 - a + planes].reshape(planes * width, 3 * wide1), b1[a])
    grad = grad.astype(BF16)
    grad = jnp.concatenate([grad[p * width : (p + 1) * width] for p in range(planes)], axis=1)
    turn = order_matrix(d.half, planes, d.height)
    out[...] = lax.dot_general(turn, grad, (((1,), (1,)), ((), ())), preferred_element_type=F32).astype(BF16)


def final_kernel(d, *refs):
    member = lax.axis_index("chan")
    parts, (out1, out2) = refs[:-2], refs[-2:]
    terms = [p[...].astype(F32) for p in parts]
    while len(terms) > 1:
        terms = [terms[i] + terms[i + 1] for i in range(0, len(terms), 2)]
    total = terms[0]
    half = d.half

    def lay_out(base, groups, chans, out):
        full = groups * chans
        for tile in range(4):
            rows = [total[base + (g * 4 + tile) * chans : base + (g * 4 + tile + 1) * chans] for g in range(groups)]
            rows = jnp.concatenate(rows, axis=0) if groups > 1 else rows[0]
            flat = pltpu.roll(rows, member * (full // 2), 0).T
            spots = [(2 * tile, b, b) for b in range(3)] + [(2 * tile + 1, b, 3 + b) for b in range(3)]
            spots += {0: [(8, 0, 6), (8, 1, 7)], 1: [(8, 2, 6)]}.get(tile, [])
            for m, b, spot in spots:
                tap = 9 * (m // 3) + 3 * b + m % 3
                out[tap * half : (tap + 1) * half, :] = flat[spot * half : (spot + 1) * half]

    lay_out(0, 1, d.mid, out1)
    lay_out(4 * d.mid, 2, d.half2, out2)


class Sizes:
    pass


def shards(feats, weight_one, weight_two, cotangent):
    d = Sizes()
    slabs = lax.axis_size("depth")
    assert lax.axis_size("chan") == 2 and slabs % BLOCK == 0
    d.half, d.planes, d.height, d.width = feats.shape
    d.half2, coarse, d.height2, width2 = cotangent.shape
    d.mid = weight_one.shape[0]
    assert d.planes == 2 and coarse == 1 and d.half * 8 == 128 and d.height2 * d.half2 == 128
    assert d.width == 128 and d.height == 8 and d.mid == 32
    blocks = slabs // BLOCK
    per = BLOCK * d.planes
    wide1 = d.height * d.mid
    own1 = d.height * d.half
    wide2 = d.height2 * 2 * d.half2
    zl = d.height2 * d.mid

    def call(kernel, outs, scratch=(), flops=0, ins=None, mib=40, aliases=None):
        def run(*args):
            return pl.pallas_call(
                functools.partial(kernel, d),
                out_shape=[jax.ShapeDtypeStruct(shape, dtype) for shape, dtype in outs],
                in_specs=[pl.BlockSpec(memory_space=ins or pltpu.VMEM)] * len(args),
                out_specs=[VMEM] * len(outs),
                scratch_shapes=list(scratch),
                input_output_aliases=aliases or {},
                compiler_params=pltpu.CompilerParams(vmem_limit_bytes=mib << 20),
                cost_estimate=pl.CostEstimate(flops=flops, bytes_accessed=1 << 20, transcendentals=0),
            )(*args)

        return run

    rows = d.planes * d.width + width2
    feats_shape = (d.half * d.planes * d.height, d.width)
    (item,) = call(
        pack_kernel,
        [((rows, 128), BF16)],
        [
            pltpu.VMEM(feats_shape, BF16),
            pltpu.VMEM((d.half2 * d.height2, width2), BF16),
            pltpu.SemaphoreType.DMA((2,)),
        ],
        ins=pltpu.HBM,
        mib=24,
    )(feats.reshape(feats_shape), cotangent.reshape(-1, width2))

    def xor(x, k):
        return lax.ppermute(x, "depth", [(i, i ^ k) for i in range(slabs)])

    def gather(k):
        return xor(item, k)

    def swap(x):
        return lax.ppermute(x, "chan", [(0, 1), (1, 0)])

    side_rows = EDGE * d.width + 2 * width2
    mid, to_a, to_b = call(
        sort_kernel, [((BLOCK * rows, 128), BF16), ((side_rows, 128), BF16), ((side_rows, 128), BF16)]
    )(item, *[gather(k) for k in range(1, BLOCK)])
    pair_a = [(i, i ^ BLOCK) for i in range(slabs)]
    inside = range(BLOCK, slabs - BLOCK)
    pair_b = [(i, ((i - BLOCK) ^ BLOCK) + BLOCK if i in inside else i) for i in range(slabs)]

    def trade(x_a, x_b):
        a = lax.ppermute(x_a, "depth", pair_a)
        b = lax.ppermute(x_b, "depth", pair_b)
        return a, b

    a, b = trade(to_a, to_b)
    mid_x, a_x, b_x = swap(mid), swap(a), swap(b)

    w1 = jnp.transpose(weight_one, (2, 0, 1)).reshape(27 * d.mid, d.mid)
    w2 = jnp.transpose(weight_two, (2, 1, 0)).reshape(27 * d.mid, 2 * d.half2)
    f1, b1, f2, b2 = call(
        weight_kernel,
        [
            ((3, 6 * own1, wide1), BF16),
            ((3, 3 * wide1, own1), BF16),
            ((3, 3 * zl, wide2), BF16),
            ((3, 3 * wide2, wide1), BF16),
        ],
        [
            pltpu.VMEM(w1.shape, BF16),
            pltpu.VMEM(w2.shape, BF16),
            pltpu.VMEM((27 * d.mid, wide1), BF16),
            pltpu.VMEM((27 * d.mid, own1), BF16),
            pltpu.VMEM((27 * d.mid, wide2), BF16),
            pltpu.VMEM((27 * 2 * d.half2, wide1), BF16),
            pltpu.SemaphoreType.DMA((2,)),
        ],
        flops=1 << 30,
        ins=pltpu.HBM,
        mib=24,
    )(w1, w2)
    xs_mid, xs_mid_x, slopes_mid, rows_mid, pooled = call(
        middle_kernel,
        [
            ((per + 2 * EDGE, d.width, 3 * own1), BF16),
            ((per + 2 * EDGE, d.width, 3 * own1), BF16),
            ((per - 2, d.width, wide1), F32),
            ((per - 2, d.width, zl), F32),
            ((BLOCK - 2, width2, zl), BF16),
        ],
        [pltpu.VMEM((BLOCK - 2, d.width, zl), F32)],
        flops=1 << 30,
    )(mid, mid_x, f1)
    pooled_a, pooled_b = trade(pooled, pooled)
    xs, _, slopes_out, rows_out = call(
        outer_kernel,
        [
            ((per + 2 * EDGE, d.width, 3 * own1), BF16),
            ((per + 2 * EDGE, d.width, 3 * own1), BF16),
            ((6, d.width, wide1), F32),
            ((6, d.width, zl), F32),
        ],
        flops=1 << 30,
        aliases={4: 0, 5: 1},
    )(a, b, a_x, b_x, xs_mid, xs_mid_x, f1)

    grads, sums = call(
        main_kernel,
        [((d.planes + 2, d.width, wide1), BF16), ((4 * d.mid + 8 * d.half2, 128), BF16)],
        [
            pltpu.VMEM((BLOCK + 4, width2, wide2), BF16),
            pltpu.VMEM((per + 4, d.width, wide1), F32),
            pltpu.VMEM((per + 4, d.width, zl), F32),
            pltpu.VMEM((3 * BLOCK - 2, d.width, zl), F32),
            pltpu.VMEM((3 * BLOCK - 2, width2, 3 * zl), BF16),
            pltpu.VMEM((BLOCK + 4, width2, 3 * wide2), BF16),
            pltpu.VMEM(((BLOCK + 2) * (wide1 // 128), d.width, 128), F32),
            pltpu.VMEM((per + 2, d.width, wide1), BF16),
        ],
        flops=1 << 32,
    )(a, mid, b, a_x, mid_x, b_x, xs, slopes_mid, rows_mid, slopes_out, rows_out, pooled_a, pooled, pooled_b, f2, b2)

    parts = [sums]
    radix = 1
    while radix < blocks:
        fan = min(4, blocks // radix)
        mine = parts[0] if len(parts) == 1 else sum_parts(parts)
        parts = [mine] + [xor(mine, BLOCK * radix * k) for k in range(1, fan)]
        radix *= fan
    (grad,) = call(
        feats_kernel, [(feats_shape, BF16)], [pltpu.VMEM((d.planes + 2, d.width, 3 * wide1), BF16)], flops=1 << 30
    )(grads, b1)
    out1, out2 = call(final_kernel, [((27 * d.half, d.mid), F32), ((27 * d.half, 2 * d.half2), F32)])(*parts)
    return (
        grad.reshape(feats.shape),
        out1.reshape(27, d.half, d.mid).transpose(2, 1, 0),
        out2.reshape(27, d.half, 2 * d.half2).transpose(2, 1, 0),
    )


def sum_parts(parts):
    terms = [p.astype(F32) for p in parts]
    while len(terms) > 1:
        terms = [terms[i] + terms[i + 1] for i in range(0, len(terms), 2)]
    return terms[0].astype(BF16)


def solution(mesh):
    return jax.shard_map(
        shards,
        mesh=mesh,
        in_specs=(P("chan", "depth", None, None), P(), P(), P("chan", "depth", None, None)),
        out_specs=(P("chan", "depth", None, None), P(None, "chan", None), P(None, "chan", None)),
        check_vma=False,
    )
```

```python
import functools

import jax
import jax.numpy as jnp
from jax import lax
from jax.experimental import pallas as pl
from jax.experimental.pallas import tpu as pltpu
from jax.sharding import PartitionSpec as P

F32 = jnp.float32
BF16 = jnp.bfloat16
BLOCK = 4
EDGE = 3
VMEM = pl.BlockSpec(memory_space=pltpu.VMEM)


def log2(n):
    assert n & (n - 1) == 0
    return n.bit_length() - 1


def digits(index, *sizes):
    out = []
    for size in reversed(sizes):
        out.append(index & (size - 1))
        index = index >> log2(size)
    return out[::-1]


def iotas(rows, cols):
    return (
        lax.broadcasted_iota(jnp.int32, (rows, cols), 0),
        lax.broadcasted_iota(jnp.int32, (rows, cols), 1),
    )


def one_hot(condition, value=1.0):
    return jnp.where(condition, value, 0.0).astype(BF16)


def mm(a, b):
    return jnp.dot(a, b, preferred_element_type=F32)


def mm_t(a, b):
    return lax.dot_general(a, b, (((0,), (0,)), ((), ())), preferred_element_type=F32)


def order_matrix(chans, planes, height):
    size = chans * planes * height
    k, n = iotas(size, size)
    chan, plane, row = digits(k, chans, planes, height)
    return one_hot(n == (plane * height + row) * chans + chan)


def shifted(x):
    rows = x.shape[0]
    at = lax.broadcasted_iota(jnp.int32, x.shape, 0)
    before = jnp.where(at == 0, 0.0, pltpu.roll(x, 1, 0))
    after = jnp.where(at == rows - 1, 0.0, pltpu.roll(x, rows - 1, 0))
    return before, after


def sigmoid(x):
    return 0.5 + 0.5 * jnp.tanh(0.5 * x)


def slope_of(pre, sig):
    return sig * (1.0 + pre * (1.0 - sig))


def pack_kernel(d, feats, cot, out, feats_in, cot_in, sems):
    copies = [
        pltpu.make_async_copy(feats, feats_in, sems.at[0]),
        pltpu.make_async_copy(cot, cot_in, sems.at[1]),
    ]
    for copy in copies:
        copy.start()
    planes, width = d.planes, d.width
    lanes = d.height * d.half
    turn = order_matrix(d.half, planes, d.height)
    turn2 = order_matrix(d.half2, 1, d.height2)
    copies[0].wait()
    f = mm_t(feats_in[...], turn).astype(BF16)
    for p in range(planes):
        out[p * width : (p + 1) * width, :] = f[:, p * lanes : (p + 1) * lanes]
    copies[1].wait()
    out[planes * width :, :] = mm_t(cot_in[...], turn2).astype(BF16)


def parity():
    return (lax.axis_index("depth") >> log2(BLOCK)) & 1 == 0


def sort_kernel(d, i0, i1, i2, i3, mid, to_a, to_b):
    place = lax.axis_index("depth") & (BLOCK - 1)
    odd = (lax.axis_index("depth") >> log2(BLOCK)) & 1
    width, width2 = d.width, d.width // 2
    body = d.planes * width
    per = BLOCK * body
    for k, ref in enumerate((i0, i1, i2, i3)):
        at = place ^ k
        mid[pl.ds(at * body, body), :] = ref[:body, :]
        mid[pl.ds(per + at * width2, width2), :] = ref[body:, :]
    side = EDGE * width
    for out, top in ((to_a, 1 - odd), (to_b, odd)):
        out[:side, :] = mid[pl.ds(pl.multiple_of(top * (per - side), side // EDGE), side), :]
        out[side:, :] = mid[pl.ds(pl.multiple_of(per + top * 2 * width2, width2), 2 * width2), :]


def band(out, a, at, size, groups, row, shift):
    strip = jnp.zeros((size, row.shape[1]), BF16)
    for b in range(3):
        strip = jnp.where(row == shift[b], groups[b], strip)
    out[a, at : at + size, :] = strip


def weight_kernel(d, w1, w2, f1, b1, f2, b2, w1_in, w2_in, t1, t2, t3, t4, sems):
    copies = [pltpu.make_async_copy(w1, w1_in, sems.at[0]), pltpu.make_async_copy(w2, w2_in, sems.at[1])]
    for copy in copies:
        copy.start()
    member = lax.axis_index("chan")
    mid, half, half2 = d.mid, d.half, d.half2
    h1, h2 = d.height, d.height2
    wide1 = h1 * mid
    own1 = h1 * half
    wide2 = h2 * 2 * half2
    k, n = iotas(mid, wide1)
    own_first = (k ^ (member * half)) == (n & (mid - 1))
    for copy in copies:
        copy.wait()
    for t in range(27):
        at = slice(t * mid, (t + 1) * mid)
        t1[at, :] = mm_t(w1_in[at, :], one_hot(own_first)).astype(BF16)
        t4[t * 2 * half2 : (t + 1) * 2 * half2, :] = mm_t(w2_in[at, :], one_hot(own_first, 0.125)).astype(BF16)
    k, n = iotas(mid, own1)
    t2[...] = mm(w1_in[...], one_hot((k ^ (member * half)) == (n & (half - 1)))).astype(BF16)
    k, n = iotas(2 * half2, wide2)
    g2, _, o2 = digits(n, 2, h2, half2)
    t3[...] = mm(w2_in[...], one_hot((k ^ (member * half2)) == g2 * half2 + o2)).astype(BF16)

    def rows_of(ref, a, c, size, total, group):
        at = [(9 * a + 3 * b + c) * total + (group ^ member) * size for b in range(3)]
        return [ref[pl.ds(pl.multiple_of(x, size), size), :] for x in at]

    row1 = lax.broadcasted_iota(jnp.int32, (half, wide1), 1) >> log2(mid)
    row2 = lax.broadcasted_iota(jnp.int32, (half, own1), 1) >> log2(half)
    row3 = digits(lax.broadcasted_iota(jnp.int32, (half, wide2), 1), 2, h2, half2)[1]
    row4 = lax.broadcasted_iota(jnp.int32, (half2, wide1), 1) >> (log2(mid) + 1)
    for a in range(3):
        for c in range(3):
            for g in range(2):
                tiles = rows_of(t1, a, c, half, mid, g)
                for r in range(h1):
                    band(f1, a, (g * 3 + c) * own1 + r * half, half, tiles, row1, (r + 1, r, r - 1))
                tiles = rows_of(t2, a, c, half, mid, g)
                for r in range(h1):
                    at = (c * h1 + r) * mid + g * half
                    band(b1, a, at, half, tiles, row2, (r - 1, r, r + 1))
                tiles = rows_of(t3, a, c, half, mid, g)
                for r in range(h2):
                    at = ((c * 2 + g) * h2 + r) * half
                    band(f2, a, at, half, tiles, row3, (r + 1, r, r - 1))
                tiles = rows_of(t4, a, c, half2, 2 * half2, g)
                for r in range(h2):
                    at = ((c * 2 + g) * h2 + r) * half2
                    band(b2, a, at, half2, tiles, row4, (r - 1, r, r + 1))


def spread_plane(d, x, xs, q):
    lanes = d.height * d.half
    before, after = shifted(x.astype(F32))
    xs[q, :, 0:lanes] = before.astype(BF16)
    xs[q, :, lanes : 2 * lanes] = x
    xs[q, :, 2 * lanes :] = after.astype(BF16)


def pool_matrix(d):
    k, n = iotas(d.height * d.mid, d.height2 * d.mid)
    r, o = digits(k, d.height, d.mid)
    g, i = digits(o, 2, d.half)
    return one_hot(n == (g * d.height2 + (r >> 1)) * d.half + i, 0.125)


def stacked(ref, starts, count):
    tall = [ref[q : q + count].reshape(count * ref.shape[1], ref.shape[2]) for q in starts]
    return tall[0] if len(tall) == 1 else jnp.concatenate(tall, axis=0)


def first_conv(d, halves, starts, count, f1):
    size = 3 * d.height * d.half
    pre = jnp.zeros((len(starts) * count * d.width, d.height * d.mid), F32)
    for g, ref in enumerate(halves):
        for a in range(3):
            pre = pre + mm(stacked(ref, [q + a - 1 for q in starts], count), f1[a, g * size : (g + 1) * size])
    return pre


def first_level(d, pre, count, pool, slopes, rows, at):
    sig = sigmoid(pre)
    slopes[at : at + count] = slope_of(pre, sig).reshape(count, d.width, -1)
    rows[at : at + count] = mm((pre * sig).astype(BF16), pool).reshape(count, d.width, -1)


def pool_pair(d, rows, at, pair, k):
    width2 = d.width // 2
    pair[k] = rows[at] + rows[at + 1]
    return pair[k, pl.ds(0, width2, 2), :] + pair[k, pl.ds(1, width2, 2), :]


def pick(lower, even, a, b, outside):
    value = jnp.where(even, b, a) if lower else jnp.where(even, a, b)
    return jnp.where(outside, jnp.zeros_like(value), value)


def ends():
    place = lax.axis_index("depth")
    return place < BLOCK, place >= lax.axis_size("depth") - BLOCK


def middle_kernel(d, mi, mi_x, f1, xs, xs_x, slopes, rows, pooled, pair):
    per = BLOCK * d.planes
    for p in range(per):
        at = slice(p * d.width, (p + 1) * d.width)
        spread_plane(d, mi[at, :], xs, EDGE + p)
        spread_plane(d, mi_x[at, :], xs_x, EDGE + p)
    pool = pool_matrix(d)
    pre = first_conv(d, (xs, xs_x), [EDGE + 1], per - 2, f1)
    first_level(d, pre, per - 2, pool, slopes, rows, 0)
    for u in range(BLOCK - 2):
        pooled[u] = pool_pair(d, rows, 2 * u + 1, pair, u).astype(BF16)


def outer_kernel(d, a, b, a_x, b_x, xs_in, xs_x_in, f1, xs, xs_x, slopes, rows):
    del xs_in, xs_x_in
    per = BLOCK * d.planes
    even = parity()
    first, last = ends()
    for pair, ref in (((a, b), xs), ((a_x, b_x), xs_x)):
        for p in range(EDGE):
            x, y = (r[p * d.width : (p + 1) * d.width, :] for r in pair)
            spread_plane(d, pick(True, even, x, y, first), ref, p)
            spread_plane(d, pick(False, even, x, y, last), ref, EDGE + per + p)
    pool = pool_matrix(d)
    pre = first_conv(d, (xs, xs_x), [1, per + EDGE - 1], 3, f1)
    first_level(d, pre, 6, pool, slopes, rows, 0)


def spread_cell(cell, zs, u):
    lanes = cell.shape[1]
    before, after = shifted(cell)
    zs[u, :, 0:lanes] = before.astype(BF16)
    zs[u, :, lanes : 2 * lanes] = cell.astype(BF16)
    zs[u, :, 2 * lanes :] = after.astype(BF16)


def spread_grad(cell, gs, u):
    lanes = cell.shape[1]
    before, after = shifted(cell)
    gs[u, :, 0:lanes] = after.astype(BF16)
    gs[u, :, lanes : 2 * lanes] = cell.astype(BF16)
    gs[u, :, 2 * lanes :] = before.astype(BF16)


def second_conv(zs, starts, count, f2):
    pre = None
    for a in range(3):
        part = mm(stacked(zs, [q + a - 1 for q in starts], count), f2[a])
        pre = part if pre is None else pre + part
    return pre


def collect(d, parts, groups, height, chans, tiles, first_slot):
    lane = lax.broadcasted_iota(jnp.int32, (chans, 128), 1)
    tap_row = lane >> log2(d.half)
    slots = 128 // d.half
    for g in range(groups):
        for m in range(9):
            value = jnp.zeros((chans, 128), F32)
            for r in range(height):
                at = (g * height + r) * chans
                tile = parts[m // 3][at : at + chans, (m % 3) * 128 : (m % 3 + 1) * 128]
                tile = pltpu.roll(tile, (1 - r) * d.half % 128, 1)
                if r == 0:
                    tile = jnp.where(tap_row == 0, 0.0, tile)
                if r == height - 1:
                    tile = jnp.where(tap_row == 2, 0.0, tile)
                value += tile
            slot = first_slot + 27 * g + 3 * m
            t, spot = slot // slots, slot % slots
            if spot:
                value = pltpu.roll(value, spot * d.half, 1)
            here = (tap_row >= spot) & (tap_row < spot + 3)
            tiles[t] = jnp.where(here, value, tiles.get(t, 0.0))
            if spot + 3 > slots:
                tiles[t + 1] = jnp.where(tap_row < spot + 3 - slots, value, 0.0)


def second_kernel(d, mi, mi_x, pooled, rows_mid, rows_out, f2, zs, gs, sums, pair):
    per, width = BLOCK * d.planes, d.width
    width2 = width // 2
    wide2 = d.height2 * 2 * d.half2
    first, last = ends()
    low = pool_pair(d, [rows_out[0], rows_out[1]], 0, pair, 0)
    spread_cell(jnp.where(first, 0.0, low), zs, 0)
    spread_cell(pool_pair(d, [rows_out[2], rows_mid[0]], 0, pair, 1), zs, 1)
    for u in range(BLOCK - 2):
        spread_cell(pooled[u].astype(F32), zs, 2 + u)
    spread_cell(pool_pair(d, [rows_mid[per - 3], rows_out[3]], 0, pair, 2), zs, BLOCK)
    high = pool_pair(d, [rows_out[4], rows_out[5]], 0, pair, 3)
    spread_cell(jnp.where(last, 0.0, high), zs, BLOCK + 1)
    pre = second_conv(zs, [1], BLOCK, f2)
    slope = slope_of(pre, sigmoid(pre))
    for u in range(BLOCK):
        at = slice(per * width + u * width2, per * width + (u + 1) * width2)
        cot = jnp.concatenate([mi[at, :], mi_x[at, :]], axis=1).astype(F32)
        spread_grad(cot * slope[u * width2 : (u + 1) * width2], gs, u)
    center = gs[:, :, wide2 : 2 * wide2].reshape(BLOCK * width2, wide2)
    parts = [mm_t(center, stacked(zs, [a], BLOCK)) for a in range(3)]
    tiles = {}
    collect(d, parts, 2, d.height2, d.half2, tiles, 0)
    for t, tile in tiles.items():
        sums[t * d.half2 : (t + 1) * d.half2, :] = tile.astype(BF16)


def main_kernel(
    d, a, b, a_x, b_x, xs, slopes_mid, slopes_out, pooled_a, pooled_b, zs_in, gs_in, sums_in, f2, b2,
    grads_out, late, sums_out, zs, gs, up, g1,
):
    place = lax.axis_index("depth")
    first, last = ends()
    even = parity()
    planes, width, wide1 = d.planes, d.width, d.height * d.mid
    width2 = width // 2
    wide2 = d.height2 * 2 * d.half2
    per = BLOCK * planes
    side = EDGE * width

    zs[2 : 4 + BLOCK] = zs_in[...]
    gs[2 : 2 + BLOCK] = gs_in[...]
    for k in range(2):
        spread_cell(pick(True, even, pooled_a[k], pooled_b[k], first).astype(F32), zs, k)
        spread_cell(pick(False, even, pooled_a[k], pooled_b[k], last).astype(F32), zs, 4 + BLOCK + k)
    pre = second_conv(zs, [1, 3 + BLOCK], 2, f2)
    slope = slope_of(pre, sigmoid(pre))
    for k in range(4):
        at = slice(side + (k % 2) * width2, side + (k % 2 + 1) * width2)
        lower = k < 2
        cot = [pick(lower, even, x[at, :], y[at, :], first if lower else last) for x, y in ((a, b), (a_x, b_x))]
        cot = jnp.concatenate(cot, axis=1).astype(F32)
        spread_grad(cot * slope[k * width2 : (k + 1) * width2], gs, k if lower else BLOCK + k)

    inner = BLOCK + 2
    back = None
    for t in range(3):
        part = mm(gs[2 - t : 2 - t + inner].reshape(inner * width2, 3 * wide2), b2[t])
        back = part if back is None else back + part
    pieces = wide1 // 128
    for u in range(inner):
        x = back[u * width2 : (u + 1) * width2]
        for piece in range(pieces):
            lanes = slice(piece * 128, (piece + 1) * 128)
            up[u * pieces + piece, pl.ds(0, width2, 2), :] = x[:, lanes]
            up[u * pieces + piece, pl.ds(1, width2, 2), :] = x[:, lanes]
    for u in range(per + 2):
        q = per - 1 + u
        both = [up[(q - 6) // 2 * pieces + piece] for piece in range(pieces)]
        if q <= per:
            slope = slopes_out[q - per + 2]
        elif q >= 2 * per - 1:
            slope = slopes_out[q - 2 * per + 4]
        else:
            slope = slopes_mid[q - per - 1]
        g = jnp.concatenate(both, axis=1) * slope
        if q < per:
            g = jnp.where(first, 0.0, g)
        if q >= 2 * per:
            g = jnp.where(last, 0.0, g)
        g1[u] = g.astype(BF16)

    center = g1[1 : 1 + per].reshape(per * width, wide1)
    parts = [mm_t(center, stacked(xs, [EDGE + t - 1], per)) for t in range(3)]
    tiles = {}
    collect(d, parts, 1, d.height, d.mid, tiles, 0)
    kept = sums_in.shape[0]
    sums_out[:kept, :] = sums_in[...]
    for t, tile in tiles.items():
        late[t * d.mid : (t + 1) * d.mid, :] = tile.astype(BF16)
    sums_out[kept:, :] = late[...]
    grads_out[...] = g1[pl.ds((place & (BLOCK - 1)) * planes, planes + 2)]


def feats_kernel(d, g1, b1, out, wide):
    planes, width, wide1 = d.planes, d.width, d.height * d.mid
    for u in range(planes + 2):
        g = g1[u]
        before, after = shifted(g.astype(F32))
        wide[u, :, 0:wide1] = after.astype(BF16)
        wide[u, :, wide1 : 2 * wide1] = g
        wide[u, :, 2 * wide1 :] = before.astype(BF16)
    grad = jnp.zeros((planes * width, d.height * d.half), F32)
    for a in range(3):
        grad += mm(wide[2 - a : 2 - a + planes].reshape(planes * width, 3 * wide1), b1[a])
    grad = grad.astype(BF16)
    grad = jnp.concatenate([grad[p * width : (p + 1) * width] for p in range(planes)], axis=1)
    turn = order_matrix(d.half, planes, d.height)
    out[...] = lax.dot_general(turn, grad, (((1,), (1,)), ((), ())), preferred_element_type=F32).astype(BF16)


def final_kernel(d, *refs):
    swapped = lax.axis_index("chan") == 1
    parts, (out1, out2, r) = list(refs[:-3]), refs[-3:]
    rows = parts[0].shape[0]
    terms = []
    while parts:
        pieces = [parts.pop(0)[...].astype(F32)]
        while sum(piece.shape[0] for piece in pieces) < rows:
            pieces.append(parts.pop(0)[...].astype(F32))
        terms.append(pieces[0] if len(pieces) == 1 else jnp.concatenate(pieces, axis=0))
    while len(terms) > 1:
        terms = [terms[i] + terms[i + 1] for i in range(0, len(terms), 2)]
    total = terms[0]
    half, mid = d.half, d.mid
    slots = 128 // half
    for t in range(total.shape[0] // mid):
        flat = total[t * mid : (t + 1) * mid].T
        for spot in range(slots):
            early = -(-2 * 27 // slots)
            slot = slots * t + spot if t < early else slots * (t - early) + spot + 2 * 27
            if slot >= (2 * 27 if t < early else 3 * 27):
                continue
            g, m, b = slot // 27, slot % 27 // 3, slot % 3
            tap = 9 * (m // 3) + 3 * b + m % 3
            r[g, tap * half : (tap + 1) * half, :] = flat[spot * half : (spot + 1) * half]
    x, y = r[0], r[1]
    out2[...] = jnp.concatenate([jnp.where(swapped, y, x), jnp.where(swapped, x, y)], axis=1)
    x = r[2]
    out1[...] = jnp.where(swapped, jnp.concatenate([x[:, half:], x[:, :half]], axis=1), x)


class Sizes:
    pass


def shards(feats, weight_one, weight_two, cotangent):
    d = Sizes()
    slabs = lax.axis_size("depth")
    assert lax.axis_size("chan") == 2 and slabs % BLOCK == 0
    d.half, d.planes, d.height, d.width = feats.shape
    d.half2, coarse, d.height2, width2 = cotangent.shape
    d.mid = weight_one.shape[0]
    assert d.planes == 2 and coarse == 1 and d.half * 8 == 128 and d.height2 * d.half2 == 128
    assert d.width == 128 and d.height == 8 and d.mid == d.half2 == 32
    blocks = slabs // BLOCK
    per = BLOCK * d.planes
    wide1 = d.height * d.mid
    own1 = d.height * d.half
    wide2 = d.height2 * 2 * d.half2
    zl = d.height2 * d.mid

    def call(kernel, outs, scratch=(), flops=0, ins=None, mib=40, aliases=None):
        def run(*args):
            return pl.pallas_call(
                functools.partial(kernel, d),
                out_shape=[jax.ShapeDtypeStruct(shape, dtype) for shape, dtype in outs],
                in_specs=[pl.BlockSpec(memory_space=ins or pltpu.VMEM)] * len(args),
                out_specs=[VMEM] * len(outs),
                scratch_shapes=list(scratch),
                input_output_aliases=aliases or {},
                compiler_params=pltpu.CompilerParams(vmem_limit_bytes=mib << 20),
                cost_estimate=pl.CostEstimate(flops=flops, bytes_accessed=1 << 20, transcendentals=0),
            )(*args)

        return run

    rows = d.planes * d.width + width2
    feats_shape = (d.half * d.planes * d.height, d.width)
    (item,) = call(
        pack_kernel,
        [((rows, 128), BF16)],
        [
            pltpu.VMEM(feats_shape, BF16),
            pltpu.VMEM((d.half2 * d.height2, width2), BF16),
            pltpu.SemaphoreType.DMA((2,)),
        ],
        ins=pltpu.HBM,
        mib=24,
    )(feats.reshape(feats_shape), cotangent.reshape(-1, width2))

    def xor(x, k):
        return lax.ppermute(x, "depth", [(i, i ^ k) for i in range(slabs)])

    def gather(k):
        return xor(item, k)

    def swap(x):
        return lax.ppermute(x, "chan", [(0, 1), (1, 0)])

    side_rows = EDGE * d.width + 2 * width2
    mid, to_a, to_b = call(
        sort_kernel, [((BLOCK * rows, 128), BF16), ((side_rows, 128), BF16), ((side_rows, 128), BF16)]
    )(item, *[gather(k) for k in range(1, BLOCK)])
    pair_a = [(i, i ^ BLOCK) for i in range(slabs)]
    inside = range(BLOCK, slabs - BLOCK)
    pair_b = [(i, ((i - BLOCK) ^ BLOCK) + BLOCK if i in inside else i) for i in range(slabs)]

    def trade(x_a, x_b):
        a = lax.ppermute(x_a, "depth", pair_a)
        b = lax.ppermute(x_b, "depth", pair_b)
        return a, b

    a, b = trade(to_a, to_b)
    mid_x, a_x, b_x = swap(mid), swap(a), swap(b)

    w1 = jnp.transpose(weight_one, (2, 0, 1)).reshape(27 * d.mid, d.mid)
    w2 = jnp.transpose(weight_two, (2, 1, 0)).reshape(27 * d.mid, 2 * d.half2)
    f1, b1, f2, b2 = call(
        weight_kernel,
        [
            ((3, 6 * own1, wide1), BF16),
            ((3, 3 * wide1, own1), BF16),
            ((3, 3 * zl, wide2), BF16),
            ((3, 3 * wide2, wide1), BF16),
        ],
        [
            pltpu.VMEM(w1.shape, BF16),
            pltpu.VMEM(w2.shape, BF16),
            pltpu.VMEM((27 * d.mid, wide1), BF16),
            pltpu.VMEM((27 * d.mid, own1), BF16),
            pltpu.VMEM((27 * d.mid, wide2), BF16),
            pltpu.VMEM((27 * 2 * d.half2, wide1), BF16),
            pltpu.SemaphoreType.DMA((2,)),
        ],
        flops=1 << 30,
        ins=pltpu.HBM,
        mib=24,
    )(w1, w2)
    xs_mid, xs_mid_x, slopes_mid, rows_mid, pooled = call(
        middle_kernel,
        [
            ((per + 2 * EDGE, d.width, 3 * own1), BF16),
            ((per + 2 * EDGE, d.width, 3 * own1), BF16),
            ((per - 2, d.width, wide1), F32),
            ((per - 2, d.width, zl), F32),
            ((BLOCK - 2, width2, zl), BF16),
        ],
        [pltpu.VMEM((BLOCK - 2, d.width, zl), F32)],
        flops=1 << 30,
    )(mid, mid_x, f1)
    pooled_a, pooled_b = trade(pooled, pooled)
    xs, _, slopes_out, rows_out = call(
        outer_kernel,
        [
            ((per + 2 * EDGE, d.width, 3 * own1), BF16),
            ((per + 2 * EDGE, d.width, 3 * own1), BF16),
            ((6, d.width, wide1), F32),
            ((6, d.width, zl), F32),
        ],
        flops=1 << 30,
        aliases={4: 0, 5: 1},
    )(a, b, a_x, b_x, xs_mid, xs_mid_x, f1)

    fan = min(4, blocks)

    def move(x, k):
        return xor(x, BLOCK * k)

    early_rows, late_rows = -(-2 * 27 // 8) * d.half2, -(-27 // 8) * d.mid
    zs, gs, early = call(
        second_kernel,
        [
            ((BLOCK + 2, width2, 3 * zl), BF16),
            ((BLOCK, width2, 3 * wide2), BF16),
            ((early_rows, 128), BF16),
        ],
        [pltpu.VMEM((BLOCK, d.width, zl), F32)],
        flops=1 << 30,
    )(mid, mid_x, pooled, rows_mid, rows_out, f2)
    early = [early] + [move(early, k) for k in range(2, fan)]
    grads, late, sums = call(
        main_kernel,
        [
            ((d.planes + 2, d.width, wide1), BF16),
            ((late_rows, 128), BF16),
            ((early_rows + late_rows, 128), BF16),
        ],
        [
            pltpu.VMEM((3 * BLOCK - 2, width2, 3 * zl), BF16),
            pltpu.VMEM((BLOCK + 4, width2, 3 * wide2), BF16),
            pltpu.VMEM(((BLOCK + 2) * (wide1 // 128), d.width, 128), F32),
            pltpu.VMEM((per + 2, d.width, wide1), BF16),
        ],
        flops=1 << 32,
    )(a, b, a_x, b_x, xs, slopes_mid, slopes_out, pooled_a, pooled_b, zs, gs, early[0], f2, b2)

    parts = [(sums,)]
    for k in range(fan - 1, 1, -1):
        parts.append((early[k - 1], move(late, k)))
    if fan > 1:
        parts.append((move(sums, 1),))
    parts = [parts[i] for i in (0, -1, -2, -3)[: len(parts)]]
    radix = fan
    while radix < blocks:
        whole = [p[0] if len(p) == 1 else jnp.concatenate(p) for p in parts]
        mine = sum_parts(whole)
        fan = min(4, blocks // radix)
        parts = [(mine,)] + [(xor(mine, BLOCK * radix * k),) for k in range(1, fan)]
        radix *= fan
    parts = sum(parts, ())
    (grad,) = call(
        feats_kernel, [(feats_shape, BF16)], [pltpu.VMEM((d.planes + 2, d.width, 3 * wide1), BF16)], flops=1 << 30
    )(grads, b1)
    out1, out2 = call(
        final_kernel,
        [((27 * d.half, d.mid), F32), ((27 * d.half, 2 * d.half2), F32)],
        [pltpu.VMEM((3, 27 * d.half, d.mid), F32)],
    )(*parts)
    return (
        grad.reshape(feats.shape),
        out1.reshape(27, d.half, d.mid).transpose(2, 1, 0),
        out2.reshape(27, d.half, 2 * d.half2).transpose(2, 1, 0),
    )


def sum_parts(parts):
    terms = [p.astype(F32) for p in parts]
    while len(terms) > 1:
        terms = [terms[i] + terms[i + 1] for i in range(0, len(terms), 2)]
    return terms[0].astype(BF16)


def solution(mesh):
    return jax.shard_map(
        shards,
        mesh=mesh,
        in_specs=(P("chan", "depth", None, None), P(), P(), P("chan", "depth", None, None)),
        out_specs=(P("chan", "depth", None, None), P(None, "chan", None), P(None, "chan", None)),
        check_vma=False,
    )
```

```python
import functools

import jax
import jax.numpy as jnp
from jax import lax
from jax.experimental import pallas as pl
from jax.experimental.pallas import tpu as pltpu
from jax.sharding import PartitionSpec as P

F32 = jnp.float32
BF16 = jnp.bfloat16
BLOCK = 4
EDGE = 3
VMEM = pl.BlockSpec(memory_space=pltpu.VMEM)


def log2(n):
    assert n & (n - 1) == 0
    return n.bit_length() - 1


def digits(index, *sizes):
    out = []
    for size in reversed(sizes):
        out.append(index & (size - 1))
        index = index >> log2(size)
    return out[::-1]


def iotas(rows, cols):
    return (
        lax.broadcasted_iota(jnp.int32, (rows, cols), 0),
        lax.broadcasted_iota(jnp.int32, (rows, cols), 1),
    )


def one_hot(condition, value=1.0):
    return jnp.where(condition, value, 0.0).astype(BF16)


def mm(a, b):
    return jnp.dot(a, b, preferred_element_type=F32)


def mm_t(a, b):
    return lax.dot_general(a, b, (((0,), (0,)), ((), ())), preferred_element_type=F32)


def order_matrix(chans, planes, height):
    size = chans * planes * height
    k, n = iotas(size, size)
    chan, plane, row = digits(k, chans, planes, height)
    return one_hot(n == (plane * height + row) * chans + chan)


def shifted(x):
    rows = x.shape[0]
    at = lax.broadcasted_iota(jnp.int32, x.shape, 0)
    before = jnp.where(at == 0, 0.0, pltpu.roll(x, 1, 0))
    after = jnp.where(at == rows - 1, 0.0, pltpu.roll(x, rows - 1, 0))
    return before, after


def sigmoid(x):
    return 0.5 + 0.5 * jnp.tanh(0.5 * x)


def slope_of(pre, sig):
    return sig * (1.0 + pre * (1.0 - sig))


def pack_kernel(d, raw, out):
    planes, width = d.planes, d.width
    lanes = d.height * d.half
    rows = planes * lanes
    f = mm_t(raw[:rows, :], order_matrix(d.half, planes, d.height)).astype(BF16)
    for p in range(planes):
        out[p * width : (p + 1) * width, :] = f[:, p * lanes : (p + 1) * lanes]
    c = mm_t(raw[rows:, :], order_matrix(d.half2, 1, d.height2)).astype(BF16)
    out[planes * width :, :] = c[: width // 2]


def parity():
    return (lax.axis_index("depth") >> log2(BLOCK)) & 1 == 0


def sort_kernel(d, i0, i1, i2, i3, mid, to_a, to_b):
    place = lax.axis_index("depth") & (BLOCK - 1)
    odd = (lax.axis_index("depth") >> log2(BLOCK)) & 1
    width, width2 = d.width, d.width // 2
    body = d.planes * width
    per = BLOCK * body
    for k, ref in enumerate((i0, i1, i2, i3)):
        at = place ^ k
        mid[pl.ds(at * body, body), :] = ref[:body, :]
        mid[pl.ds(per + at * width2, width2), :] = ref[body:, :]
    side = EDGE * width
    for out, top in ((to_a, 1 - odd), (to_b, odd)):
        out[...] = mid[pl.ds(pl.multiple_of(top * (per - side), width), side), :]


def band(out, a, at, size, groups, row, shift):
    strip = jnp.zeros((size, row.shape[1]), BF16)
    for b in range(3):
        strip = jnp.where(row == shift[b], groups[b], strip)
    out[a, at : at + size, :] = strip


def weight_kernel(d, w1, w2, f1, b1, f2, b2, w1_in, w2_in, t1, t2, t3, t4, sems):
    copies = [pltpu.make_async_copy(w1, w1_in, sems.at[0]), pltpu.make_async_copy(w2, w2_in, sems.at[1])]
    for copy in copies:
        copy.start()
    member = lax.axis_index("chan")
    mid, half, half2 = d.mid, d.half, d.half2
    h1, h2 = d.height, d.height2
    wide1 = h1 * mid
    own1 = h1 * half
    wide2 = h2 * 2 * half2
    k, n = iotas(mid, wide1)
    own_first = (k ^ (member * half)) == (n & (mid - 1))
    for copy in copies:
        copy.wait()
    for t in range(27):
        at = slice(t * mid, (t + 1) * mid)
        t1[at, :] = mm_t(w1_in[at, :], one_hot(own_first)).astype(BF16)
        t4[t * 2 * half2 : (t + 1) * 2 * half2, :] = mm_t(w2_in[at, :], one_hot(own_first, 0.125)).astype(BF16)
    k, n = iotas(mid, own1)
    t2[...] = mm(w1_in[...], one_hot((k ^ (member * half)) == (n & (half - 1)))).astype(BF16)
    k, n = iotas(2 * half2, wide2)
    g2, _, o2 = digits(n, 2, h2, half2)
    t3[...] = mm(w2_in[...], one_hot((k ^ (member * half2)) == g2 * half2 + o2)).astype(BF16)

    def rows_of(ref, a, c, size, total, group):
        at = [(9 * a + 3 * b + c) * total + (group ^ member) * size for b in range(3)]
        return [ref[pl.ds(pl.multiple_of(x, size), size), :] for x in at]

    row1 = lax.broadcasted_iota(jnp.int32, (half, wide1), 1) >> log2(mid)
    row2 = lax.broadcasted_iota(jnp.int32, (half, own1), 1) >> log2(half)
    row3 = digits(lax.broadcasted_iota(jnp.int32, (half, wide2), 1), 2, h2, half2)[1]
    row4 = lax.broadcasted_iota(jnp.int32, (half2, wide1), 1) >> (log2(mid) + 1)
    for a in range(3):
        for c in range(3):
            for g in range(2):
                tiles = rows_of(t1, a, c, half, mid, g)
                for r in range(h1):
                    band(f1, a, (g * 3 + c) * own1 + r * half, half, tiles, row1, (r + 1, r, r - 1))
                tiles = rows_of(t2, a, c, half, mid, g)
                for r in range(h1):
                    at = (c * h1 + r) * mid + g * half
                    band(b1, a, at, half, tiles, row2, (r - 1, r, r + 1))
                tiles = rows_of(t3, a, c, half, mid, g)
                for r in range(h2):
                    at = ((c * 2 + g) * h2 + r) * half
                    band(f2, a, at, half, tiles, row3, (r + 1, r, r - 1))
                tiles = rows_of(t4, a, c, half2, 2 * half2, g)
                for r in range(h2):
                    at = ((c * 2 + g) * h2 + r) * half2
                    band(b2, a, at, half2, tiles, row4, (r - 1, r, r + 1))


def spread_plane(d, x, xs, q):
    lanes = d.height * d.half
    before, after = shifted(x.astype(F32))
    xs[q, :, 0:lanes] = before.astype(BF16)
    xs[q, :, lanes : 2 * lanes] = x
    xs[q, :, 2 * lanes :] = after.astype(BF16)


def pool_matrix(d):
    k, n = iotas(d.height * d.mid, d.height2 * d.mid)
    r, o = digits(k, d.height, d.mid)
    g, i = digits(o, 2, d.half)
    return one_hot(n == (g * d.height2 + (r >> 1)) * d.half + i, 0.125)


def stacked(ref, starts, count):
    tall = [ref[q : q + count].reshape(count * ref.shape[1], ref.shape[2]) for q in starts]
    return tall[0] if len(tall) == 1 else jnp.concatenate(tall, axis=0)


def first_conv(d, halves, starts, count, f1, pre=None):
    size = 3 * d.height * d.half
    for g, ref in enumerate(halves):
        for a in range(3 if ref is not None else 0):
            term = mm(stacked(ref, [q + a - 1 for q in starts], count), f1[a, g * size : (g + 1) * size])
            pre = term if pre is None else pre + term
    return pre


def first_level(d, pre, count, pool, slopes, rows, at):
    sig = sigmoid(pre)
    slopes[at : at + count] = slope_of(pre, sig).reshape(count, d.width, -1)
    rows[at : at + count] = mm((pre * sig).astype(BF16), pool).reshape(count, d.width, -1)


def pool_pair(d, rows, at, pair, k):
    width2 = d.width // 2
    pair[k] = rows[at] + rows[at + 1]
    return pair[k, pl.ds(0, width2, 2), :] + pair[k, pl.ds(1, width2, 2), :]


def pick(lower, even, a, b, outside):
    value = jnp.where(even, b, a) if lower else jnp.where(even, a, b)
    return jnp.where(outside, jnp.zeros_like(value), value)


def ends():
    place = lax.axis_index("depth")
    return place < BLOCK, place >= lax.axis_size("depth") - BLOCK


def middle_kernel(d, mi, mi_x, f1, xs, xs_x, slopes, rows, for_a, for_b, pair):
    per = BLOCK * d.planes
    for p in range(per):
        at = slice(p * d.width, (p + 1) * d.width)
        spread_plane(d, mi[at, :], xs, EDGE + p)
        spread_plane(d, mi_x[at, :], xs_x, EDGE + p)
    pool = pool_matrix(d)
    pre = first_conv(d, (xs, xs_x), [EDGE + 1], per - 2, f1)
    first_level(d, pre, per - 2, pool, slopes, rows, 0)
    width2 = d.width // 2
    odd = (lax.axis_index("depth") >> log2(BLOCK)) & 1
    for u in range(2):
        cell = pool_pair(d, rows, 2 * u + 1, pair, u).astype(BF16)
        for out, top in ((for_a, 1 - odd), (for_b, odd)):
            out[u * width2 : (u + 1) * width2, :] = cell
            for g, ref in enumerate((mi, mi_x)):
                at = pl.multiple_of(per * d.width + (top * (BLOCK - 2) + u) * width2, width2)
                to = (2 + 2 * g + u) * width2
                out[to : to + width2, :] = ref[pl.ds(at, width2), :]


def spread_ends(d, a, b, xs):
    even = parity()
    first, last = ends()
    for p in range(EDGE):
        x, y = (r[p * d.width : (p + 1) * d.width, :] for r in (a, b))
        spread_plane(d, pick(True, even, x, y, first), xs, p)
        spread_plane(d, pick(False, even, x, y, last), xs, EDGE + BLOCK * d.planes + p)


def outer_kernel(d, a, b, xs_in, f1, xs, part):
    del xs_in
    spread_ends(d, a, b, xs)
    part[...] = first_conv(d, (xs, None), [1, BLOCK * d.planes + EDGE - 1], 3, f1)


def close_kernel(d, a, b, xs_in, f1, part, xs, slopes, rows):
    del xs_in
    spread_ends(d, a, b, xs)
    pre = first_conv(d, (None, xs), [1, BLOCK * d.planes + EDGE - 1], 3, f1, part[...])
    first_level(d, pre, 6, pool_matrix(d), slopes, rows, 0)


def spread_cell(cell, zs, u):
    lanes = cell.shape[1]
    before, after = shifted(cell)
    zs[u, :, 0:lanes] = before.astype(BF16)
    zs[u, :, lanes : 2 * lanes] = cell.astype(BF16)
    zs[u, :, 2 * lanes :] = after.astype(BF16)


def spread_grad(cell, gs, u):
    lanes = cell.shape[1]
    before, after = shifted(cell)
    gs[u, :, 0:lanes] = after.astype(BF16)
    gs[u, :, lanes : 2 * lanes] = cell.astype(BF16)
    gs[u, :, 2 * lanes :] = before.astype(BF16)


def second_conv(zs, starts, count, f2):
    pre = None
    for a in range(3):
        part = mm(stacked(zs, [q + a - 1 for q in starts], count), f2[a])
        pre = part if pre is None else pre + part
    return pre


def collect(d, parts, groups, height, chans, tiles, first_slot):
    lane = lax.broadcasted_iota(jnp.int32, (chans, 128), 1)
    tap_row = lane >> log2(d.half)
    slots = 128 // d.half
    for g in range(groups):
        for m in range(9):
            value = jnp.zeros((chans, 128), F32)
            for r in range(height):
                at = (g * height + r) * chans
                tile = parts[m // 3][at : at + chans, (m % 3) * 128 : (m % 3 + 1) * 128]
                tile = pltpu.roll(tile, (1 - r) * d.half % 128, 1)
                if r == 0:
                    tile = jnp.where(tap_row == 0, 0.0, tile)
                if r == height - 1:
                    tile = jnp.where(tap_row == 2, 0.0, tile)
                value += tile
            slot = first_slot + 27 * g + 3 * m
            t, spot = slot // slots, slot % slots
            if spot:
                value = pltpu.roll(value, spot * d.half, 1)
            here = (tap_row >= spot) & (tap_row < spot + 3)
            tiles[t] = jnp.where(here, value, tiles.get(t, 0.0))
            if spot + 3 > slots:
                tiles[t + 1] = jnp.where(tap_row < spot + 3 - slots, value, 0.0)


def second_kernel(d, mi, mi_x, pooled, rows_mid, rows_out, f2, zs, gs, sums, pair):
    per, width = BLOCK * d.planes, d.width
    width2 = width // 2
    wide2 = d.height2 * 2 * d.half2
    first, last = ends()
    low = pool_pair(d, [rows_out[0], rows_out[1]], 0, pair, 0)
    spread_cell(jnp.where(first, 0.0, low), zs, 0)
    spread_cell(pool_pair(d, [rows_out[2], rows_mid[0]], 0, pair, 1), zs, 1)
    for u in range(BLOCK - 2):
        spread_cell(pooled[u * width2 : (u + 1) * width2, :].astype(F32), zs, 2 + u)
    spread_cell(pool_pair(d, [rows_mid[per - 3], rows_out[3]], 0, pair, 2), zs, BLOCK)
    high = pool_pair(d, [rows_out[4], rows_out[5]], 0, pair, 3)
    spread_cell(jnp.where(last, 0.0, high), zs, BLOCK + 1)
    pre = second_conv(zs, [1], BLOCK, f2)
    slope = slope_of(pre, sigmoid(pre))
    for u in range(BLOCK):
        at = slice(per * width + u * width2, per * width + (u + 1) * width2)
        cot = jnp.concatenate([mi[at, :], mi_x[at, :]], axis=1).astype(F32)
        spread_grad(cot * slope[u * width2 : (u + 1) * width2], gs, u)
    center = gs[:, :, wide2 : 2 * wide2].reshape(BLOCK * width2, wide2)
    parts = [mm_t(center, stacked(zs, [a], BLOCK)) for a in range(3)]
    tiles = {}
    collect(d, parts, 2, d.height2, d.half2, tiles, 0)
    for t, tile in tiles.items():
        sums[t * d.half2 : (t + 1) * d.half2, :] = tile.astype(BF16)


def main_kernel(
    d, xs, slopes_mid, slopes_out, from_a, from_b, zs_in, gs_in, sums_in, f2, b2,
    grads_out, late, sums_out, zs, gs, up, g1,
):
    place = lax.axis_index("depth")
    first, last = ends()
    even = parity()
    planes, width, wide1 = d.planes, d.width, d.height * d.mid
    width2 = width // 2
    wide2 = d.height2 * 2 * d.half2
    per = BLOCK * planes

    def adjacent(lower, k):
        at = slice(k * width2, (k + 1) * width2)
        return pick(lower, even, from_a[at, :], from_b[at, :], first if lower else last)

    zs[2 : 4 + BLOCK] = zs_in[...]
    gs[2 : 2 + BLOCK] = gs_in[...]
    for k in range(2):
        spread_cell(adjacent(True, k).astype(F32), zs, k)
        spread_cell(adjacent(False, k).astype(F32), zs, 4 + BLOCK + k)
    pre = second_conv(zs, [1, 3 + BLOCK], 2, f2)
    slope = slope_of(pre, sigmoid(pre))
    for k in range(4):
        lower = k < 2
        cot = jnp.concatenate([adjacent(lower, 2 + 2 * g + k % 2) for g in range(2)], axis=1).astype(F32)
        spread_grad(cot * slope[k * width2 : (k + 1) * width2], gs, k if lower else BLOCK + k)

    inner = BLOCK + 2
    back = None
    for t in range(3):
        part = mm(gs[2 - t : 2 - t + inner].reshape(inner * width2, 3 * wide2), b2[t])
        back = part if back is None else back + part
    pieces = wide1 // 128
    for u in range(inner):
        x = back[u * width2 : (u + 1) * width2]
        for piece in range(pieces):
            lanes = slice(piece * 128, (piece + 1) * 128)
            up[u * pieces + piece, pl.ds(0, width2, 2), :] = x[:, lanes]
            up[u * pieces + piece, pl.ds(1, width2, 2), :] = x[:, lanes]
    for u in range(per + 2):
        q = per - 1 + u
        both = [up[(q - 6) // 2 * pieces + piece] for piece in range(pieces)]
        if q <= per:
            slope = slopes_out[q - per + 2]
        elif q >= 2 * per - 1:
            slope = slopes_out[q - 2 * per + 4]
        else:
            slope = slopes_mid[q - per - 1]
        g = jnp.concatenate(both, axis=1) * slope
        if q < per:
            g = jnp.where(first, 0.0, g)
        if q >= 2 * per:
            g = jnp.where(last, 0.0, g)
        g1[u] = g.astype(BF16)

    center = g1[1 : 1 + per].reshape(per * width, wide1)
    parts = [mm_t(center, stacked(xs, [EDGE + t - 1], per)) for t in range(3)]
    tiles = {}
    collect(d, parts, 1, d.height, d.mid, tiles, 0)
    kept = sums_in.shape[0]
    sums_out[:kept, :] = sums_in[...]
    for t, tile in tiles.items():
        late[t * d.mid : (t + 1) * d.mid, :] = tile.astype(BF16)
    sums_out[kept:, :] = late[...]
    grads_out[...] = g1[pl.ds((place & (BLOCK - 1)) * planes, planes + 2)]


def feats_kernel(d, g1, b1, out, wide):
    planes, width, wide1 = d.planes, d.width, d.height * d.mid
    for u in range(planes + 2):
        g = g1[u]
        before, after = shifted(g.astype(F32))
        wide[u, :, 0:wide1] = after.astype(BF16)
        wide[u, :, wide1 : 2 * wide1] = g
        wide[u, :, 2 * wide1 :] = before.astype(BF16)
    grad = jnp.zeros((planes * width, d.height * d.half), F32)
    for a in range(3):
        grad += mm(wide[2 - a : 2 - a + planes].reshape(planes * width, 3 * wide1), b1[a])
    grad = grad.astype(BF16)
    grad = jnp.concatenate([grad[p * width : (p + 1) * width] for p in range(planes)], axis=1)
    turn = order_matrix(d.half, planes, d.height)
    out[...] = lax.dot_general(turn, grad, (((1,), (1,)), ((), ())), preferred_element_type=F32).astype(BF16)


def final_kernel(d, *refs):
    swapped = lax.axis_index("chan") == 1
    parts, (out1, out2, r) = list(refs[:-3]), refs[-3:]
    rows = parts[0].shape[0]
    terms = []
    while parts:
        pieces = [parts.pop(0)[...].astype(F32)]
        while sum(piece.shape[0] for piece in pieces) < rows:
            pieces.append(parts.pop(0)[...].astype(F32))
        terms.append(pieces[0] if len(pieces) == 1 else jnp.concatenate(pieces, axis=0))
    while len(terms) > 1:
        terms = [terms[i] + terms[i + 1] for i in range(0, len(terms), 2)]
    total = terms[0]
    half, mid = d.half, d.mid
    slots = 128 // half
    for t in range(total.shape[0] // mid):
        flat = total[t * mid : (t + 1) * mid].T
        for spot in range(slots):
            early = -(-2 * 27 // slots)
            slot = slots * t + spot if t < early else slots * (t - early) + spot + 2 * 27
            if slot >= (2 * 27 if t < early else 3 * 27):
                continue
            g, m, b = slot // 27, slot % 27 // 3, slot % 3
            tap = 9 * (m // 3) + 3 * b + m % 3
            r[g, tap * half : (tap + 1) * half, :] = flat[spot * half : (spot + 1) * half]
    x, y = r[0], r[1]
    out2[...] = jnp.concatenate([jnp.where(swapped, y, x), jnp.where(swapped, x, y)], axis=1)
    x = r[2]
    out1[...] = jnp.where(swapped, jnp.concatenate([x[:, half:], x[:, :half]], axis=1), x)


class Sizes:
    pass


def shards(feats, weight_one, weight_two, cotangent):
    d = Sizes()
    slabs = lax.axis_size("depth")
    assert lax.axis_size("chan") == 2 and slabs % BLOCK == 0
    d.half, d.planes, d.height, d.width = feats.shape
    d.half2, coarse, d.height2, width2 = cotangent.shape
    d.mid = weight_one.shape[0]
    assert d.planes == 2 and coarse == 1 and d.half * 8 == 128 and d.height2 * d.half2 == 128
    assert d.width == 128 and d.height == 8 and d.mid == d.half2 == 32
    blocks = slabs // BLOCK
    per = BLOCK * d.planes
    wide1 = d.height * d.mid
    own1 = d.height * d.half
    wide2 = d.height2 * 2 * d.half2
    zl = d.height2 * d.mid

    def call(kernel, outs, scratch=(), flops=0, ins=None, mib=40, aliases=None):
        def run(*args):
            return pl.pallas_call(
                functools.partial(kernel, d),
                out_shape=[jax.ShapeDtypeStruct(shape, dtype) for shape, dtype in outs],
                in_specs=[pl.BlockSpec(memory_space=ins or pltpu.VMEM)] * len(args),
                out_specs=[VMEM] * len(outs),
                scratch_shapes=list(scratch),
                input_output_aliases=aliases or {},
                compiler_params=pltpu.CompilerParams(vmem_limit_bytes=mib << 20),
                cost_estimate=pl.CostEstimate(flops=flops, bytes_accessed=1 << 20, transcendentals=0),
            )(*args)

        return run

    rows = d.planes * d.width + width2
    feats_shape = (d.half * d.planes * d.height, d.width)
    cells = jnp.pad(cotangent.reshape(-1, width2), ((0, 0), (0, d.width - width2)))
    raw = jnp.concatenate([feats.reshape(feats_shape), cells])
    (item,) = call(pack_kernel, [((rows, 128), BF16)])(raw)

    def xor(x, k):
        return lax.ppermute(x, "depth", [(i, i ^ k) for i in range(slabs)])

    def gather(k):
        return xor(item, k)

    def swap(x):
        return lax.ppermute(x, "chan", [(0, 1), (1, 0)])

    side_rows = EDGE * d.width
    mid, to_a, to_b = call(
        sort_kernel,
        [((BLOCK * rows, 128), BF16), ((side_rows, 128), BF16), ((side_rows, 128), BF16)],
    )(item, *[gather(k) for k in range(1, BLOCK)])
    pair_a = [(i, i ^ BLOCK) for i in range(slabs)]
    inside = range(BLOCK, slabs - BLOCK)
    pair_b = [(i, ((i - BLOCK) ^ BLOCK) + BLOCK if i in inside else i) for i in range(slabs)]

    def trade(x_a, x_b):
        a = lax.ppermute(x_a, "depth", pair_a)
        b = lax.ppermute(x_b, "depth", pair_b)
        return a, b

    a, b = trade(to_a, to_b)
    mid_x, a_x, b_x = swap(mid), swap(a), swap(b)

    w1 = jnp.transpose(weight_one, (2, 0, 1)).reshape(27 * d.mid, d.mid)
    w2 = jnp.transpose(weight_two, (2, 1, 0)).reshape(27 * d.mid, 2 * d.half2)
    f1, b1, f2, b2 = call(
        weight_kernel,
        [
            ((3, 6 * own1, wide1), BF16),
            ((3, 3 * wide1, own1), BF16),
            ((3, 3 * zl, wide2), BF16),
            ((3, 3 * wide2, wide1), BF16),
        ],
        [
            pltpu.VMEM(w1.shape, BF16),
            pltpu.VMEM(w2.shape, BF16),
            pltpu.VMEM((27 * d.mid, wide1), BF16),
            pltpu.VMEM((27 * d.mid, own1), BF16),
            pltpu.VMEM((27 * d.mid, wide2), BF16),
            pltpu.VMEM((27 * 2 * d.half2, wide1), BF16),
            pltpu.SemaphoreType.DMA((2,)),
        ],
        flops=1 << 30,
        ins=pltpu.HBM,
        mib=24,
    )(w1, w2)
    xs_mid, xs_mid_x, slopes_mid, rows_mid, for_a, for_b = call(
        middle_kernel,
        [
            ((per + 2 * EDGE, d.width, 3 * own1), BF16),
            ((per + 2 * EDGE, d.width, 3 * own1), BF16),
            ((per - 2, d.width, wide1), F32),
            ((per - 2, d.width, zl), F32),
            ((6 * width2, zl), BF16),
            ((6 * width2, zl), BF16),
        ],
        [pltpu.VMEM((BLOCK - 2, d.width, zl), F32)],
        flops=1 << 30,
    )(mid, mid_x, f1)
    from_a, from_b = trade(for_a, for_b)
    ends_shape = (6 * d.width, wide1)
    xs, part = call(
        outer_kernel,
        [((per + 2 * EDGE, d.width, 3 * own1), BF16), (ends_shape, F32)],
        flops=1 << 30,
        aliases={2: 0},
    )(a, b, xs_mid, f1)
    _, slopes_out, rows_out = call(
        close_kernel,
        [
            ((per + 2 * EDGE, d.width, 3 * own1), BF16),
            ((6, d.width, wide1), F32),
            ((6, d.width, zl), F32),
        ],
        flops=1 << 30,
        aliases={2: 0},
    )(a_x, b_x, xs_mid_x, f1, part)

    fan = min(4, blocks)

    def move(x, k):
        return xor(x, BLOCK * k)

    early_rows, late_rows = -(-2 * 27 // 8) * d.half2, -(-27 // 8) * d.mid
    zs, gs, early = call(
        second_kernel,
        [
            ((BLOCK + 2, width2, 3 * zl), BF16),
            ((BLOCK, width2, 3 * wide2), BF16),
            ((early_rows, 128), BF16),
        ],
        [pltpu.VMEM((BLOCK, d.width, zl), F32)],
        flops=1 << 30,
    )(mid, mid_x, for_a, rows_mid, rows_out, f2)
    early = [early] + [move(early, k) for k in range(2, fan)]
    grads, late, sums = call(
        main_kernel,
        [
            ((d.planes + 2, d.width, wide1), BF16),
            ((late_rows, 128), BF16),
            ((early_rows + late_rows, 128), BF16),
        ],
        [
            pltpu.VMEM((3 * BLOCK - 2, width2, 3 * zl), BF16),
            pltpu.VMEM((BLOCK + 4, width2, 3 * wide2), BF16),
            pltpu.VMEM(((BLOCK + 2) * (wide1 // 128), d.width, 128), F32),
            pltpu.VMEM((per + 2, d.width, wide1), BF16),
        ],
        flops=1 << 32,
    )(xs, slopes_mid, slopes_out, from_a, from_b, zs, gs, early[0], f2, b2)

    parts = [(sums,)]
    for k in range(fan - 1, 1, -1):
        parts.append((early[k - 1], move(late, k)))
    if fan > 1:
        parts.append((move(sums, 1),))
    parts = [parts[i] for i in (0, -1, -2, -3)[: len(parts)]]
    radix = fan
    while radix < blocks:
        whole = [p[0] if len(p) == 1 else jnp.concatenate(p) for p in parts]
        mine = sum_parts(whole)
        fan = min(4, blocks // radix)
        parts = [(mine,)] + [(xor(mine, BLOCK * radix * k),) for k in range(1, fan)]
        radix *= fan
    parts = sum(parts, ())
    (grad,) = call(
        feats_kernel,
        [(feats_shape, BF16)],
        [pltpu.VMEM((d.planes + 2, d.width, 3 * wide1), BF16)],
        flops=1 << 30,
    )(grads, b1)
    out1, out2 = call(
        final_kernel,
        [((27 * d.half, d.mid), F32), ((27 * d.half, 2 * d.half2), F32)],
        [pltpu.VMEM((3, 27 * d.half, d.mid), F32)],
    )(*parts)
    return (
        grad.reshape(feats.shape),
        out1.reshape(27, d.half, d.mid).transpose(2, 1, 0),
        out2.reshape(27, d.half, 2 * d.half2).transpose(2, 1, 0),
    )


def sum_parts(parts):
    terms = [p.astype(F32) for p in parts]
    while len(terms) > 1:
        terms = [terms[i] + terms[i + 1] for i in range(0, len(terms), 2)]
    return terms[0].astype(BF16)


def solution(mesh):
    return jax.shard_map(
        shards,
        mesh=mesh,
        in_specs=(P("chan", "depth", None, None), P(), P(), P("chan", "depth", None, None)),
        out_specs=(P("chan", "depth", None, None), P(None, "chan", None), P(None, "chan", None)),
        check_vma=False,
    )
```

```python
import functools

import jax
import jax.numpy as jnp
from jax import lax
from jax.experimental import pallas as pl
from jax.experimental.pallas import tpu as pltpu
from jax.sharding import PartitionSpec as P

F32 = jnp.float32
BF16 = jnp.bfloat16
BLOCK = 4
EDGE = 3
VMEM = pl.BlockSpec(memory_space=pltpu.VMEM)


def log2(n):
    assert n & (n - 1) == 0
    return n.bit_length() - 1


def digits(index, *sizes):
    out = []
    for size in reversed(sizes):
        out.append(index & (size - 1))
        index = index >> log2(size)
    return out[::-1]


def iotas(rows, cols):
    return (
        lax.broadcasted_iota(jnp.int32, (rows, cols), 0),
        lax.broadcasted_iota(jnp.int32, (rows, cols), 1),
    )


def one_hot(condition, value=1.0):
    return jnp.where(condition, value, 0.0).astype(BF16)


def mm(a, b):
    return jnp.dot(a, b, preferred_element_type=F32)


def mm_t(a, b):
    return lax.dot_general(a, b, (((0,), (0,)), ((), ())), preferred_element_type=F32)


def order_matrix(chans, planes, height):
    size = chans * planes * height
    k, n = iotas(size, size)
    chan, plane, row = digits(k, chans, planes, height)
    return one_hot(n == (plane * height + row) * chans + chan)


def shifted(x):
    rows = x.shape[0]
    at = lax.broadcasted_iota(jnp.int32, x.shape, 0)
    before = jnp.where(at == 0, 0.0, pltpu.roll(x, 1, 0))
    after = jnp.where(at == rows - 1, 0.0, pltpu.roll(x, rows - 1, 0))
    return before, after


def sigmoid(x):
    return 0.5 + 0.5 * jnp.tanh(0.5 * x)


def slope_of(pre, sig):
    return sig * (1.0 + pre * (1.0 - sig))


def pack_kernel(d, raw, out):
    planes, width = d.planes, d.width
    lanes = d.height * d.half
    rows = planes * lanes
    f = mm_t(raw[:rows, :], order_matrix(d.half, planes, d.height)).astype(BF16)
    for p in range(planes):
        out[p * width : (p + 1) * width, :] = f[:, p * lanes : (p + 1) * lanes]
    c = mm_t(raw[rows:, :], order_matrix(d.half2, 1, d.height2)).astype(BF16)
    out[planes * width :, :] = c[: width // 2]


def parity():
    return (lax.axis_index("depth") >> log2(BLOCK)) & 1 == 0


def sort_kernel(d, i0, i1, i2, i3, mid, to_a, to_b):
    place = lax.axis_index("depth") & (BLOCK - 1)
    odd = (lax.axis_index("depth") >> log2(BLOCK)) & 1
    width, width2 = d.width, d.width // 2
    body = d.planes * width
    per = BLOCK * body
    for k, ref in enumerate((i0, i1, i2, i3)):
        at = place ^ k
        mid[pl.ds(at * body, body), :] = ref[:body, :]
        mid[pl.ds(per + at * width2, width2), :] = ref[body:, :]
    side = EDGE * width
    for out, top in ((to_a, 1 - odd), (to_b, odd)):
        out[...] = mid[pl.ds(pl.multiple_of(top * (per - side), width), side), :]


def band(out, a, at, size, groups, row, shift):
    strip = jnp.zeros((size, row.shape[1]), BF16)
    for b in range(3):
        strip = jnp.where(row == shift[b], groups[b], strip)
    out[a, at : at + size, :] = strip


def weight_kernel(d, w1, w2, f1, b1, f2, b2, w1_in, w2_in, t1, t2, t3, t4, sems):
    copies = [pltpu.make_async_copy(w1, w1_in, sems.at[0]), pltpu.make_async_copy(w2, w2_in, sems.at[1])]
    for copy in copies:
        copy.start()
    member = lax.axis_index("chan")
    mid, half, half2 = d.mid, d.half, d.half2
    h1, h2 = d.height, d.height2
    wide1 = h1 * mid
    own1 = h1 * half
    wide2 = h2 * 2 * half2
    k, n = iotas(mid, wide1)
    own_first = (k ^ (member * half)) == (n & (mid - 1))
    for copy in copies:
        copy.wait()
    for t in range(27):
        at = slice(t * mid, (t + 1) * mid)
        t1[at, :] = mm_t(w1_in[at, :], one_hot(own_first)).astype(BF16)
        t4[t * 2 * half2 : (t + 1) * 2 * half2, :] = mm_t(w2_in[at, :], one_hot(own_first, 0.125)).astype(BF16)
    k, n = iotas(mid, own1)
    t2[...] = mm(w1_in[...], one_hot((k ^ (member * half)) == (n & (half - 1)))).astype(BF16)
    k, n = iotas(2 * half2, wide2)
    g2, _, o2 = digits(n, 2, h2, half2)
    t3[...] = mm(w2_in[...], one_hot((k ^ (member * half2)) == g2 * half2 + o2)).astype(BF16)

    def rows_of(ref, a, c, size, total, group):
        at = [(9 * a + 3 * b + c) * total + (group ^ member) * size for b in range(3)]
        return [ref[pl.ds(pl.multiple_of(x, size), size), :] for x in at]

    row1 = lax.broadcasted_iota(jnp.int32, (half, wide1), 1) >> log2(mid)
    row2 = lax.broadcasted_iota(jnp.int32, (half, own1), 1) >> log2(half)
    row3 = digits(lax.broadcasted_iota(jnp.int32, (half, wide2), 1), 2, h2, half2)[1]
    row4 = lax.broadcasted_iota(jnp.int32, (half2, wide1), 1) >> (log2(mid) + 1)
    for a in range(3):
        for c in range(3):
            for g in range(2):
                tiles = rows_of(t1, a, c, half, mid, g)
                for r in range(h1):
                    band(f1, a, (g * 3 + c) * own1 + r * half, half, tiles, row1, (r + 1, r, r - 1))
                tiles = rows_of(t2, a, c, half, mid, g)
                for r in range(h1):
                    at = (c * h1 + r) * mid + g * half
                    band(b1, a, at, half, tiles, row2, (r - 1, r, r + 1))
                tiles = rows_of(t3, a, c, half, mid, g)
                for r in range(h2):
                    at = ((c * 2 + g) * h2 + r) * half
                    band(f2, a, at, half, tiles, row3, (r + 1, r, r - 1))
                tiles = rows_of(t4, a, c, half2, 2 * half2, g)
                for r in range(h2):
                    at = ((c * 2 + g) * h2 + r) * half2
                    band(b2, a, at, half2, tiles, row4, (r - 1, r, r + 1))


def spread_plane(d, x, xs, q):
    lanes = d.height * d.half
    before, after = shifted(x.astype(F32))
    xs[q, :, 0:lanes] = before.astype(BF16)
    xs[q, :, lanes : 2 * lanes] = x
    xs[q, :, 2 * lanes :] = after.astype(BF16)


def pool_matrix(d):
    k, n = iotas(d.height * d.mid, d.height2 * d.mid)
    r, o = digits(k, d.height, d.mid)
    g, i = digits(o, 2, d.half)
    return one_hot(n == (g * d.height2 + (r >> 1)) * d.half + i, 0.125)


def stacked(ref, starts, count):
    tall = [ref[q : q + count].reshape(count * ref.shape[1], ref.shape[2]) for q in starts]
    return tall[0] if len(tall) == 1 else jnp.concatenate(tall, axis=0)


def first_conv(d, halves, starts, count, f1, pre=None):
    size = 3 * d.height * d.half
    taps = [(g, ref, a) for g, ref in enumerate(halves) if ref is not None for a in range(3)]
    fields = jnp.concatenate([stacked(ref, [q + a - 1 for q in starts], count) for g, ref, a in taps], axis=1)
    out = mm(fields, jnp.concatenate([f1[a, g * size : (g + 1) * size] for g, ref, a in taps], axis=0))
    return out if pre is None else out + pre


def first_level(d, pre, count, pool, slopes, rows, at):
    sig = sigmoid(pre)
    slopes[at : at + count] = slope_of(pre, sig).reshape(count, d.width, -1)
    rows[at : at + count] = mm((pre * sig).astype(BF16), pool).reshape(count, d.width, -1)


def pool_pair(d, rows, at, pair, k):
    width2 = d.width // 2
    pair[k] = rows[at] + rows[at + 1]
    return pair[k, pl.ds(0, width2, 2), :] + pair[k, pl.ds(1, width2, 2), :]


def pick(lower, even, a, b, outside):
    value = jnp.where(even, b, a) if lower else jnp.where(even, a, b)
    return jnp.where(outside, jnp.zeros_like(value), value)


def ends():
    place = lax.axis_index("depth")
    return place < BLOCK, place >= lax.axis_size("depth") - BLOCK


def middle_kernel(d, mi, mi_x, f1, xs, xs_x, slopes, rows, for_a, for_b, pair):
    per = BLOCK * d.planes
    for p in range(per):
        at = slice(p * d.width, (p + 1) * d.width)
        spread_plane(d, mi[at, :], xs, EDGE + p)
        spread_plane(d, mi_x[at, :], xs_x, EDGE + p)
    pool = pool_matrix(d)
    pre = first_conv(d, (xs, xs_x), [EDGE + 1], per - 2, f1)
    first_level(d, pre, per - 2, pool, slopes, rows, 0)
    width2 = d.width // 2
    odd = (lax.axis_index("depth") >> log2(BLOCK)) & 1
    for u in range(2):
        cell = pool_pair(d, rows, 2 * u + 1, pair, u).astype(BF16)
        for out, top in ((for_a, 1 - odd), (for_b, odd)):
            out[u * width2 : (u + 1) * width2, :] = cell
            for g, ref in enumerate((mi, mi_x)):
                at = pl.multiple_of(per * d.width + (top * (BLOCK - 2) + u) * width2, width2)
                to = (2 + 2 * g + u) * width2
                out[to : to + width2, :] = ref[pl.ds(at, width2), :]


def spread_ends(d, a, b, xs):
    even = parity()
    first, last = ends()
    for p in range(EDGE):
        x, y = (r[p * d.width : (p + 1) * d.width, :] for r in (a, b))
        spread_plane(d, pick(True, even, x, y, first), xs, p)
        spread_plane(d, pick(False, even, x, y, last), xs, EDGE + BLOCK * d.planes + p)


def outer_kernel(d, a, b, xs_in, f1, xs, part):
    del xs_in
    spread_ends(d, a, b, xs)
    part[...] = first_conv(d, (xs, None), [1, BLOCK * d.planes + EDGE - 1], 3, f1)


def close_kernel(d, a, b, xs_in, f1, part, xs, slopes, rows):
    del xs_in
    spread_ends(d, a, b, xs)
    pre = first_conv(d, (None, xs), [1, BLOCK * d.planes + EDGE - 1], 3, f1, part[...])
    first_level(d, pre, 6, pool_matrix(d), slopes, rows, 0)


def spread_cell(cell, zs, u):
    lanes = cell.shape[1]
    before, after = shifted(cell)
    zs[u, :, 0:lanes] = before.astype(BF16)
    zs[u, :, lanes : 2 * lanes] = cell.astype(BF16)
    zs[u, :, 2 * lanes :] = after.astype(BF16)


def spread_grad(cell, gs, u):
    lanes = cell.shape[1]
    before, after = shifted(cell)
    gs[u, :, 0:lanes] = after.astype(BF16)
    gs[u, :, lanes : 2 * lanes] = cell.astype(BF16)
    gs[u, :, 2 * lanes :] = before.astype(BF16)


def second_conv(zs, starts, count, f2):
    fields = jnp.concatenate([stacked(zs, [q + a - 1 for q in starts], count) for a in range(3)], axis=1)
    return mm(fields, f2[...].reshape(-1, f2.shape[2]))


def weight_product(center, ref, starts, count):
    fields = jnp.concatenate([stacked(ref, [q], count) for q in starts], axis=1)
    out = mm_t(center, fields)
    size = ref.shape[2]
    return [out[:, k * size : (k + 1) * size] for k in range(len(starts))]


def collect(d, parts, groups, height, chans, tiles, first_slot):
    lane = lax.broadcasted_iota(jnp.int32, (chans, 128), 1)
    tap_row = lane >> log2(d.half)
    slots = 128 // d.half
    for g in range(groups):
        for m in range(9):
            value = jnp.zeros((chans, 128), F32)
            for r in range(height):
                at = (g * height + r) * chans
                tile = parts[m // 3][at : at + chans, (m % 3) * 128 : (m % 3 + 1) * 128]
                tile = pltpu.roll(tile, (1 - r) * d.half % 128, 1)
                if r == 0:
                    tile = jnp.where(tap_row == 0, 0.0, tile)
                if r == height - 1:
                    tile = jnp.where(tap_row == 2, 0.0, tile)
                value += tile
            slot = first_slot + 27 * g + 3 * m
            t, spot = slot // slots, slot % slots
            if spot:
                value = pltpu.roll(value, spot * d.half, 1)
            here = (tap_row >= spot) & (tap_row < spot + 3)
            tiles[t] = jnp.where(here, value, tiles.get(t, 0.0))
            if spot + 3 > slots:
                tiles[t + 1] = jnp.where(tap_row < spot + 3 - slots, value, 0.0)


def second_kernel(d, mi, mi_x, pooled, rows_mid, rows_out, f2, zs, gs, sums, pair):
    per, width = BLOCK * d.planes, d.width
    width2 = width // 2
    wide2 = d.height2 * 2 * d.half2
    first, last = ends()
    low = pool_pair(d, [rows_out[0], rows_out[1]], 0, pair, 0)
    spread_cell(jnp.where(first, 0.0, low), zs, 0)
    spread_cell(pool_pair(d, [rows_out[2], rows_mid[0]], 0, pair, 1), zs, 1)
    for u in range(BLOCK - 2):
        spread_cell(pooled[u * width2 : (u + 1) * width2, :].astype(F32), zs, 2 + u)
    spread_cell(pool_pair(d, [rows_mid[per - 3], rows_out[3]], 0, pair, 2), zs, BLOCK)
    high = pool_pair(d, [rows_out[4], rows_out[5]], 0, pair, 3)
    spread_cell(jnp.where(last, 0.0, high), zs, BLOCK + 1)
    pre = second_conv(zs, [1], BLOCK, f2)
    slope = slope_of(pre, sigmoid(pre))
    for u in range(BLOCK):
        at = slice(per * width + u * width2, per * width + (u + 1) * width2)
        cot = jnp.concatenate([mi[at, :], mi_x[at, :]], axis=1).astype(F32)
        spread_grad(cot * slope[u * width2 : (u + 1) * width2], gs, u)
    center = gs[:, :, wide2 : 2 * wide2].reshape(BLOCK * width2, wide2)
    parts = weight_product(center, zs, range(3), BLOCK)
    tiles = {}
    collect(d, parts, 2, d.height2, d.half2, tiles, 0)
    for t, tile in tiles.items():
        sums[t * d.half2 : (t + 1) * d.half2, :] = tile.astype(BF16)


def main_kernel(
    d, xs, slopes_mid, slopes_out, from_a, from_b, zs_in, gs_in, f2, b2,
    grads_out, late, zs, gs, up, g1,
):
    place = lax.axis_index("depth")
    first, last = ends()
    even = parity()
    planes, width, wide1 = d.planes, d.width, d.height * d.mid
    width2 = width // 2
    per = BLOCK * planes

    def adjacent(lower, k):
        at = slice(k * width2, (k + 1) * width2)
        return pick(lower, even, from_a[at, :], from_b[at, :], first if lower else last)

    zs[2 : 4 + BLOCK] = zs_in[...]
    gs[2 : 2 + BLOCK] = gs_in[...]
    for k in range(2):
        spread_cell(adjacent(True, k).astype(F32), zs, k)
        spread_cell(adjacent(False, k).astype(F32), zs, 4 + BLOCK + k)
    pre = second_conv(zs, [1, 3 + BLOCK], 2, f2)
    slope = slope_of(pre, sigmoid(pre))
    for k in range(4):
        lower = k < 2
        cot = jnp.concatenate([adjacent(lower, 2 + 2 * g + k % 2) for g in range(2)], axis=1).astype(F32)
        spread_grad(cot * slope[k * width2 : (k + 1) * width2], gs, k if lower else BLOCK + k)

    inner = BLOCK + 2
    fields = jnp.concatenate([stacked(gs, [2 - t], inner) for t in range(3)], axis=1)
    back = mm(fields, b2[...].reshape(-1, wide1))
    pieces = wide1 // 128
    for u in range(inner):
        x = back[u * width2 : (u + 1) * width2]
        for piece in range(pieces):
            lanes = slice(piece * 128, (piece + 1) * 128)
            up[u * pieces + piece, pl.ds(0, width2, 2), :] = x[:, lanes]
            up[u * pieces + piece, pl.ds(1, width2, 2), :] = x[:, lanes]
    for u in range(per + 2):
        q = per - 1 + u
        both = [up[(q - 6) // 2 * pieces + piece] for piece in range(pieces)]
        if q <= per:
            slope = slopes_out[q - per + 2]
        elif q >= 2 * per - 1:
            slope = slopes_out[q - 2 * per + 4]
        else:
            slope = slopes_mid[q - per - 1]
        g = jnp.concatenate(both, axis=1) * slope
        if q < per:
            g = jnp.where(first, 0.0, g)
        if q >= 2 * per:
            g = jnp.where(last, 0.0, g)
        g1[u] = g.astype(BF16)

    center = g1[1 : 1 + per].reshape(per * width, wide1)
    parts = weight_product(center, xs, range(EDGE - 1, EDGE + 2), per)
    tiles = {}
    collect(d, parts, 1, d.height, d.mid, tiles, 0)
    for t, tile in tiles.items():
        late[t * d.mid : (t + 1) * d.mid, :] = tile.astype(BF16)
    grads_out[...] = g1[pl.ds((place & (BLOCK - 1)) * planes, planes + 2)]


def feats_grad(d, g1, b1, out, wide):
    planes, width, wide1 = d.planes, d.width, d.height * d.mid
    for u in range(planes + 2):
        g = g1[u]
        before, after = shifted(g.astype(F32))
        wide[u, :, 0:wide1] = after.astype(BF16)
        wide[u, :, wide1 : 2 * wide1] = g
        wide[u, :, 2 * wide1 :] = before.astype(BF16)
    fields = jnp.concatenate([stacked(wide, [2 - a], planes) for a in range(3)], axis=1)
    grad = mm(fields, b1[...].reshape(-1, d.height * d.half)).astype(BF16)
    grad = jnp.concatenate([grad[p * width : (p + 1) * width] for p in range(planes)], axis=1)
    turn = order_matrix(d.half, planes, d.height)
    out[...] = lax.dot_general(turn, grad, (((1,), (1,)), ((), ())), preferred_element_type=F32).astype(BF16)


def final_tiles(d, parts, groups):
    half, mid = d.half, d.mid
    slots = 128 // half
    for t in range(parts[0].shape[0] // mid):
        terms = [p[t * mid : (t + 1) * mid, :].astype(F32) for p in parts]
        while len(terms) > 1:
            terms = [terms[i] + terms[i + 1] for i in range(0, len(terms), 2)]
        tile = terms[0]
        if groups == 1:
            tile = pltpu.roll(tile, lax.axis_index("chan") * half, 0)
        flat = tile.T
        for slot in range(slots * t, min(slots * (t + 1), 27 * groups)):
            g, m, b = slot // 27, slot % 27 // 3, slot % 3
            spot = slot % slots
            yield g, 9 * (m // 3) + 3 * b + m % 3, flat[spot * half : (spot + 1) * half]


def fill_kernel(d, g1, b1, *refs):
    feats_out, out, wide, r = refs[-4:]
    feats_grad(d, g1, b1, feats_out, wide)
    member = lax.axis_index("chan")
    for g, tap, piece in final_tiles(d, refs[:-4], 2):
        r[g ^ member, tap * d.half : (tap + 1) * d.half, :] = piece
    out[...] = jnp.concatenate([r[0], r[1]], axis=1)


def final_kernel(d, *refs):
    out = refs[-1]
    for g, tap, piece in final_tiles(d, refs[:-1], 1):
        out[tap * d.half : (tap + 1) * d.half, :] = piece


class Sizes:
    pass


def shards(feats, weight_one, weight_two, cotangent):
    d = Sizes()
    slabs = lax.axis_size("depth")
    assert lax.axis_size("chan") == 2 and slabs % BLOCK == 0
    d.half, d.planes, d.height, d.width = feats.shape
    d.half2, coarse, d.height2, width2 = cotangent.shape
    d.mid = weight_one.shape[0]
    assert d.planes == 2 and coarse == 1 and d.half * 8 == 128 and d.height2 * d.half2 == 128
    assert d.width == 128 and d.height == 8 and d.mid == d.half2 == 32
    blocks = slabs // BLOCK
    per = BLOCK * d.planes
    wide1 = d.height * d.mid
    own1 = d.height * d.half
    wide2 = d.height2 * 2 * d.half2
    zl = d.height2 * d.mid

    def call(kernel, outs, scratch=(), flops=0, ins=None, mib=40, aliases=None):
        def run(*args):
            return pl.pallas_call(
                functools.partial(kernel, d),
                out_shape=[jax.ShapeDtypeStruct(shape, dtype) for shape, dtype in outs],
                in_specs=[pl.BlockSpec(memory_space=ins or pltpu.VMEM)] * len(args),
                out_specs=[VMEM] * len(outs),
                scratch_shapes=list(scratch),
                input_output_aliases=aliases or {},
                compiler_params=pltpu.CompilerParams(vmem_limit_bytes=mib << 20),
                cost_estimate=pl.CostEstimate(flops=flops, bytes_accessed=1 << 20, transcendentals=0),
            )(*args)

        return run

    rows = d.planes * d.width + width2
    feats_shape = (d.half * d.planes * d.height, d.width)
    cells = jnp.pad(cotangent.reshape(-1, width2), ((0, 0), (0, d.width - width2)))
    raw = jnp.concatenate([feats.reshape(feats_shape), cells])
    (item,) = call(pack_kernel, [((rows, 128), BF16)])(raw)

    def xor(x, k):
        return lax.ppermute(x, "depth", [(i, i ^ k) for i in range(slabs)])

    def gather(k):
        return xor(item, k)

    def swap(x):
        return lax.ppermute(x, "chan", [(0, 1), (1, 0)])

    side_rows = EDGE * d.width
    mid, to_a, to_b = call(
        sort_kernel, [((BLOCK * rows, 128), BF16), ((side_rows, 128), BF16), ((side_rows, 128), BF16)]
    )(item, *[gather(k) for k in range(1, BLOCK)])
    pair_a = [(i, i ^ BLOCK) for i in range(slabs)]
    inside = range(BLOCK, slabs - BLOCK)
    pair_b = [(i, ((i - BLOCK) ^ BLOCK) + BLOCK if i in inside else i) for i in range(slabs)]

    def trade(x_a, x_b):
        a = lax.ppermute(x_a, "depth", pair_a)
        b = lax.ppermute(x_b, "depth", pair_b)
        return a, b

    a, b = trade(to_a, to_b)
    mid_x, a_x, b_x = swap(mid), swap(a), swap(b)

    w1 = jnp.transpose(weight_one, (2, 0, 1)).reshape(27 * d.mid, d.mid)
    w2 = jnp.transpose(weight_two, (2, 1, 0)).reshape(27 * d.mid, 2 * d.half2)
    f1, b1, f2, b2 = call(
        weight_kernel,
        [
            ((3, 6 * own1, wide1), BF16),
            ((3, 3 * wide1, own1), BF16),
            ((3, 3 * zl, wide2), BF16),
            ((3, 3 * wide2, wide1), BF16),
        ],
        [
            pltpu.VMEM(w1.shape, BF16),
            pltpu.VMEM(w2.shape, BF16),
            pltpu.VMEM((27 * d.mid, wide1), BF16),
            pltpu.VMEM((27 * d.mid, own1), BF16),
            pltpu.VMEM((27 * d.mid, wide2), BF16),
            pltpu.VMEM((27 * 2 * d.half2, wide1), BF16),
            pltpu.SemaphoreType.DMA((2,)),
        ],
        flops=1 << 30,
        ins=pltpu.HBM,
        mib=24,
    )(w1, w2)
    xs_mid, xs_mid_x, slopes_mid, rows_mid, for_a, for_b = call(
        middle_kernel,
        [
            ((per + 2 * EDGE, d.width, 3 * own1), BF16),
            ((per + 2 * EDGE, d.width, 3 * own1), BF16),
            ((per - 2, d.width, wide1), F32),
            ((per - 2, d.width, zl), F32),
            ((6 * width2, zl), BF16),
            ((6 * width2, zl), BF16),
        ],
        [pltpu.VMEM((BLOCK - 2, d.width, zl), F32)],
        flops=1 << 30,
    )(mid, mid_x, f1)
    from_a, from_b = trade(for_a, for_b)
    ends_shape = (6 * d.width, wide1)
    xs, part = call(
        outer_kernel, [((per + 2 * EDGE, d.width, 3 * own1), BF16), (ends_shape, F32)], flops=1 << 30, aliases={2: 0}
    )(a, b, xs_mid, f1)
    _, slopes_out, rows_out = call(
        close_kernel,
        [
            ((per + 2 * EDGE, d.width, 3 * own1), BF16),
            ((6, d.width, wide1), F32),
            ((6, d.width, zl), F32),
        ],
        flops=1 << 30,
        aliases={2: 0},
    )(a_x, b_x, xs_mid_x, f1, part)

    def gather_sums(x):
        radix = 1
        parts = [x]
        while radix < blocks:
            x = sum_parts(parts)
            fan = min(4, blocks // radix)
            parts = [None] * fan
            for k in range(fan - 1, 0, -1):
                parts[k] = xor(x, BLOCK * radix * k)
            parts[0] = x
            radix *= fan
        return parts

    early_rows, late_rows = -(-2 * 27 // 8) * d.half2, -(-27 // 8) * d.mid
    zs, gs, early = call(
        second_kernel,
        [
            ((BLOCK + 2, width2, 3 * zl), BF16),
            ((BLOCK, width2, 3 * wide2), BF16),
            ((early_rows, 128), BF16),
        ],
        [pltpu.VMEM((BLOCK, d.width, zl), F32)],
        flops=1 << 30,
    )(mid, mid_x, for_a, rows_mid, rows_out, f2)
    early = gather_sums(early)
    grads, late = call(
        main_kernel,
        [
            ((d.planes + 2, d.width, wide1), BF16),
            ((late_rows, 128), BF16),
        ],
        [
            pltpu.VMEM((3 * BLOCK - 2, width2, 3 * zl), BF16),
            pltpu.VMEM((BLOCK + 4, width2, 3 * wide2), BF16),
            pltpu.VMEM(((BLOCK + 2) * (wide1 // 128), d.width, 128), F32),
            pltpu.VMEM((per + 2, d.width, wide1), BF16),
        ],
        flops=1 << 32,
    )(xs, slopes_mid, slopes_out, from_a, from_b, zs, gs, f2, b2)

    late = gather_sums(late)
    grad, out2 = call(
        fill_kernel,
        [(feats_shape, BF16), ((27 * d.half, 2 * d.half2), F32)],
        [
            pltpu.VMEM((d.planes + 2, d.width, 3 * wide1), BF16),
            pltpu.VMEM((2, 27 * d.half, d.mid), F32),
        ],
        flops=1 << 30,
    )(grads, b1, *early)
    (out1,) = call(final_kernel, [((27 * d.half, d.mid), F32)])(*late)
    return (
        grad.reshape(feats.shape),
        out1.reshape(27, d.half, d.mid).transpose(2, 1, 0),
        out2.reshape(27, d.half, 2 * d.half2).transpose(2, 1, 0),
    )


def sum_parts(parts):
    if len(parts) == 1:
        return parts[0]
    terms = [p.astype(F32) for p in parts]
    while len(terms) > 1:
        terms = [terms[i] + terms[i + 1] for i in range(0, len(terms), 2)]
    return terms[0].astype(BF16)


def solution(mesh):
    return jax.shard_map(
        shards,
        mesh=mesh,
        in_specs=(P("chan", "depth", None, None), P(), P(), P("chan", "depth", None, None)),
        out_specs=(P("chan", "depth", None, None), P(None, "chan", None), P(None, "chan", None)),
        check_vma=False,
    )
```

```python
import functools

import jax
import jax.numpy as jnp
from jax import lax
from jax.experimental import pallas as pl
from jax.experimental.pallas import tpu as pltpu
from jax.sharding import PartitionSpec as P

F32 = jnp.float32
BF16 = jnp.bfloat16
BLOCK = 4
EDGE = 3
VMEM = pl.BlockSpec(memory_space=pltpu.VMEM)


def log2(n):
    assert n & (n - 1) == 0
    return n.bit_length() - 1


def digits(index, *sizes):
    out = []
    for size in reversed(sizes):
        out.append(index & (size - 1))
        index = index >> log2(size)
    return out[::-1]


def iotas(rows, cols):
    return (
        lax.broadcasted_iota(jnp.int32, (rows, cols), 0),
        lax.broadcasted_iota(jnp.int32, (rows, cols), 1),
    )


def one_hot(condition, value=1.0):
    return jnp.where(condition, value, 0.0).astype(BF16)


def mm(a, b):
    return jnp.dot(a, b, preferred_element_type=F32)


def mm_t(a, b):
    return lax.dot_general(a, b, (((0,), (0,)), ((), ())), preferred_element_type=F32)


def order_matrix(chans, planes, height):
    size = chans * planes * height
    k, n = iotas(size, size)
    chan, plane, row = digits(k, chans, planes, height)
    return one_hot(n == (plane * height + row) * chans + chan)


def shifted(x):
    rows = x.shape[0]
    at = lax.broadcasted_iota(jnp.int32, x.shape, 0)
    before = jnp.where(at == 0, 0.0, pltpu.roll(x, 1, 0))
    after = jnp.where(at == rows - 1, 0.0, pltpu.roll(x, rows - 1, 0))
    return before, after


def sigmoid(x):
    return 0.5 + 0.5 * jnp.tanh(0.5 * x)


def slope_of(pre, sig):
    return sig * (1.0 + pre * (1.0 - sig))


def pack_kernel(d, raw, out):
    planes, width = d.planes, d.width
    lanes = d.height * d.half
    rows = planes * lanes
    f = mm_t(raw[:rows, :], order_matrix(d.half, planes, d.height)).astype(BF16)
    for p in range(planes):
        out[p * width : (p + 1) * width, :] = f[:, p * lanes : (p + 1) * lanes]
    c = mm_t(raw[rows:, :], order_matrix(d.half2, 1, d.height2)).astype(BF16)
    out[planes * width :, :] = c[: width // 2]


def parity():
    return (lax.axis_index("depth") >> log2(BLOCK)) & 1 == 0


def sort_kernel(d, i0, i1, i2, i3, mid, to_a, to_b):
    place = lax.axis_index("depth") & (BLOCK - 1)
    odd = (lax.axis_index("depth") >> log2(BLOCK)) & 1
    width, width2 = d.width, d.width // 2
    body = d.planes * width
    per = BLOCK * body
    for k, ref in enumerate((i0, i1, i2, i3)):
        at = place ^ k
        mid[pl.ds(at * body, body), :] = ref[:body, :]
        mid[pl.ds(per + at * width2, width2), :] = ref[body:, :]
    side = EDGE * width
    for out, top in ((to_a, 1 - odd), (to_b, odd)):
        out[...] = mid[pl.ds(pl.multiple_of(top * (per - side), width), side), :]


def band(out, a, at, size, groups, row, shift):
    strip = jnp.zeros((size, row.shape[1]), BF16)
    for b in range(3):
        strip = jnp.where(row == shift[b], groups[b], strip)
    out[a, at : at + size, :] = strip


def weight_kernel(d, both, f1, b1, f2, b2, t1, t2, t3, t4):
    member = lax.axis_index("chan")
    mid, half, half2 = d.mid, d.half, d.half2
    h1, h2 = d.height, d.height2
    wide1 = h1 * mid
    own1 = h1 * half
    wide2 = h2 * 2 * half2
    k, n = iotas(mid, wide1)
    own_first = (k ^ (member * half)) == (n & (mid - 1))
    w1_in, w2_in = both[: 27 * mid, :mid], both[27 * mid :, :]
    for t in range(27):
        at = slice(t * mid, (t + 1) * mid)
        t1[at, :] = mm_t(w1_in[at], one_hot(own_first)).astype(BF16)
        t4[t * 2 * half2 : (t + 1) * 2 * half2, :] = mm_t(w2_in[at], one_hot(own_first, 0.125)).astype(BF16)
    k, n = iotas(mid, own1)
    t2[...] = mm(w1_in, one_hot((k ^ (member * half)) == (n & (half - 1)))).astype(BF16)
    k, n = iotas(2 * half2, wide2)
    g2, _, o2 = digits(n, 2, h2, half2)
    t3[...] = mm(w2_in, one_hot((k ^ (member * half2)) == g2 * half2 + o2)).astype(BF16)

    def rows_of(ref, a, c, size, total, group):
        at = [(9 * a + 3 * b + c) * total + (group ^ member) * size for b in range(3)]
        return [ref[pl.ds(pl.multiple_of(x, size), size), :] for x in at]

    row1 = lax.broadcasted_iota(jnp.int32, (half, wide1), 1) >> log2(mid)
    row2 = lax.broadcasted_iota(jnp.int32, (half, own1), 1) >> log2(half)
    row3 = digits(lax.broadcasted_iota(jnp.int32, (half, wide2), 1), 2, h2, half2)[1]
    row4 = lax.broadcasted_iota(jnp.int32, (half2, wide1), 1) >> (log2(mid) + 1)
    for a in range(3):
        for c in range(3):
            for g in range(2):
                tiles = rows_of(t1, a, c, half, mid, g)
                for r in range(h1):
                    band(f1, a, (g * 3 + c) * own1 + r * half, half, tiles, row1, (r + 1, r, r - 1))
                tiles = rows_of(t2, a, c, half, mid, g)
                for r in range(h1):
                    at = (c * h1 + r) * mid + g * half
                    band(b1, a, at, half, tiles, row2, (r - 1, r, r + 1))
                tiles = rows_of(t3, a, c, half, mid, g)
                for r in range(h2):
                    at = ((c * 2 + g) * h2 + r) * half
                    band(f2, a, at, half, tiles, row3, (r + 1, r, r - 1))
                tiles = rows_of(t4, a, c, half2, 2 * half2, g)
                for r in range(h2):
                    at = ((c * 2 + g) * h2 + r) * half2
                    band(b2, a, at, half2, tiles, row4, (r - 1, r, r + 1))


def spread_plane(d, x, xs, q):
    lanes = d.height * d.half
    before, after = shifted(x.astype(F32))
    xs[q, :, 0:lanes] = before.astype(BF16)
    xs[q, :, lanes : 2 * lanes] = x
    xs[q, :, 2 * lanes :] = after.astype(BF16)


def pool_matrix(d):
    k, n = iotas(d.height * d.mid, d.height2 * d.mid)
    r, o = digits(k, d.height, d.mid)
    g, i = digits(o, 2, d.half)
    return one_hot(n == (g * d.height2 + (r >> 1)) * d.half + i, 0.125)


def stacked(ref, starts, count):
    tall = [ref[q : q + count].reshape(count * ref.shape[1], ref.shape[2]) for q in starts]
    return tall[0] if len(tall) == 1 else jnp.concatenate(tall, axis=0)


def first_conv(d, halves, starts, count, f1, pre=None):
    size = 3 * d.height * d.half
    taps = [(g, ref, a) for g, ref in enumerate(halves) if ref is not None for a in range(3)]
    fields = jnp.concatenate([stacked(ref, [q + a - 1 for q in starts], count) for g, ref, a in taps], axis=1)
    out = mm(fields, jnp.concatenate([f1[a, g * size : (g + 1) * size] for g, ref, a in taps], axis=0))
    return out if pre is None else out + pre


def first_level(d, pre, count, pool, slopes, rows, at):
    sig = sigmoid(pre)
    slopes[at : at + count] = slope_of(pre, sig).reshape(count, d.width, -1)
    rows[at : at + count] = mm((pre * sig).astype(BF16), pool).reshape(count, d.width, -1)


def pool_pair(d, rows, at, pair, k):
    width2 = d.width // 2
    pair[k] = rows[at] + rows[at + 1]
    return pair[k, pl.ds(0, width2, 2), :] + pair[k, pl.ds(1, width2, 2), :]


def pick(lower, even, a, b, outside):
    value = jnp.where(even, b, a) if lower else jnp.where(even, a, b)
    return jnp.where(outside, jnp.zeros_like(value), value)


def ends():
    place = lax.axis_index("depth")
    return place < BLOCK, place >= lax.axis_size("depth") - BLOCK


def middle_kernel(d, mi, mi_x, f1, xs, xs_x, slopes, rows, for_a, for_b, pair):
    per = BLOCK * d.planes
    for p in range(per):
        at = slice(p * d.width, (p + 1) * d.width)
        spread_plane(d, mi[at, :], xs, EDGE + p)
        spread_plane(d, mi_x[at, :], xs_x, EDGE + p)
    pool = pool_matrix(d)
    pre = first_conv(d, (xs, xs_x), [EDGE + 1], per - 2, f1)
    first_level(d, pre, per - 2, pool, slopes, rows, 0)
    width2 = d.width // 2
    odd = (lax.axis_index("depth") >> log2(BLOCK)) & 1
    for u in range(2):
        cell = pool_pair(d, rows, 2 * u + 1, pair, u).astype(BF16)
        for out, top in ((for_a, 1 - odd), (for_b, odd)):
            out[u * width2 : (u + 1) * width2, :] = cell
            for g, ref in enumerate((mi, mi_x)):
                at = pl.multiple_of(per * d.width + (top * (BLOCK - 2) + u) * width2, width2)
                to = (2 + 2 * g + u) * width2
                out[to : to + width2, :] = ref[pl.ds(at, width2), :]


def spread_ends(d, a, b, xs):
    even = parity()
    first, last = ends()
    for p in range(EDGE):
        x, y = (r[p * d.width : (p + 1) * d.width, :] for r in (a, b))
        spread_plane(d, pick(True, even, x, y, first), xs, p)
        spread_plane(d, pick(False, even, x, y, last), xs, EDGE + BLOCK * d.planes + p)


def outer_kernel(d, a, b, xs_in, f1, xs, part):
    del xs_in
    spread_ends(d, a, b, xs)
    part[...] = first_conv(d, (xs, None), [1, BLOCK * d.planes + EDGE - 1], 3, f1)


def close_kernel(d, a, b, xs_in, f1, part, xs, slopes, rows):
    del xs_in
    spread_ends(d, a, b, xs)
    pre = first_conv(d, (None, xs), [1, BLOCK * d.planes + EDGE - 1], 3, f1, part[...])
    first_level(d, pre, 6, pool_matrix(d), slopes, rows, 0)


def spread_cell(cell, zs, u):
    lanes = cell.shape[1]
    before, after = shifted(cell)
    zs[u, :, 0:lanes] = before.astype(BF16)
    zs[u, :, lanes : 2 * lanes] = cell.astype(BF16)
    zs[u, :, 2 * lanes :] = after.astype(BF16)


def spread_grad(cell, gs, u):
    lanes = cell.shape[1]
    before, after = shifted(cell)
    gs[u, :, 0:lanes] = after.astype(BF16)
    gs[u, :, lanes : 2 * lanes] = cell.astype(BF16)
    gs[u, :, 2 * lanes :] = before.astype(BF16)


def second_conv(zs, starts, count, f2):
    fields = jnp.concatenate([stacked(zs, [q + a - 1 for q in starts], count) for a in range(3)], axis=1)
    return mm(fields, f2[...].reshape(-1, f2.shape[2]))


def weight_product(center, ref, starts, count):
    fields = jnp.concatenate([stacked(ref, [q], count) for q in starts], axis=1)
    out = mm_t(center, fields)
    size = ref.shape[2]
    return [out[:, k * size : (k + 1) * size] for k in range(len(starts))]


def collect(d, parts, groups, height, chans, tiles, first_slot):
    lane = lax.broadcasted_iota(jnp.int32, (chans, 128), 1)
    tap_row = lane >> log2(d.half)
    slots = 128 // d.half
    for g in range(groups):
        for m in range(9):
            value = jnp.zeros((chans, 128), F32)
            for r in range(height):
                at = (g * height + r) * chans
                tile = parts[m // 3][at : at + chans, (m % 3) * 128 : (m % 3 + 1) * 128]
                tile = pltpu.roll(tile, (1 - r) * d.half % 128, 1)
                if r == 0:
                    tile = jnp.where(tap_row == 0, 0.0, tile)
                if r == height - 1:
                    tile = jnp.where(tap_row == 2, 0.0, tile)
                value += tile
            slot = first_slot + 27 * g + 3 * m
            t, spot = slot // slots, slot % slots
            if spot:
                value = pltpu.roll(value, spot * d.half, 1)
            here = (tap_row >= spot) & (tap_row < spot + 3)
            tiles[t] = jnp.where(here, value, tiles.get(t, 0.0))
            if spot + 3 > slots:
                tiles[t + 1] = jnp.where(tap_row < spot + 3 - slots, value, 0.0)


def second_kernel(d, mi, mi_x, pooled, rows_mid, rows_out, f2, zs, gs, sums, pair):
    per, width = BLOCK * d.planes, d.width
    width2 = width // 2
    wide2 = d.height2 * 2 * d.half2
    first, last = ends()
    low = pool_pair(d, [rows_out[0], rows_out[1]], 0, pair, 0)
    spread_cell(jnp.where(first, 0.0, low), zs, 0)
    spread_cell(pool_pair(d, [rows_out[2], rows_mid[0]], 0, pair, 1), zs, 1)
    for u in range(BLOCK - 2):
        spread_cell(pooled[u * width2 : (u + 1) * width2, :].astype(F32), zs, 2 + u)
    spread_cell(pool_pair(d, [rows_mid[per - 3], rows_out[3]], 0, pair, 2), zs, BLOCK)
    high = pool_pair(d, [rows_out[4], rows_out[5]], 0, pair, 3)
    spread_cell(jnp.where(last, 0.0, high), zs, BLOCK + 1)
    pre = second_conv(zs, [1], BLOCK, f2)
    slope = slope_of(pre, sigmoid(pre))
    for u in range(BLOCK):
        at = slice(per * width + u * width2, per * width + (u + 1) * width2)
        cot = jnp.concatenate([mi[at, :], mi_x[at, :]], axis=1).astype(F32)
        spread_grad(cot * slope[u * width2 : (u + 1) * width2], gs, u)
    center = gs[:, :, wide2 : 2 * wide2].reshape(BLOCK * width2, wide2)
    parts = weight_product(center, zs, range(3), BLOCK)
    tiles = {}
    collect(d, parts, 2, d.height2, d.half2, tiles, 0)
    for t, tile in tiles.items():
        sums[t * d.half2 : (t + 1) * d.half2, :] = tile.astype(BF16)


def main_kernel(
    d, xs, slopes_mid, slopes_out, from_a, from_b, zs_in, gs_in, f2, b2,
    grads_out, late, zs, gs, up, g1,
):
    place = lax.axis_index("depth")
    first, last = ends()
    even = parity()
    planes, width, wide1 = d.planes, d.width, d.height * d.mid
    width2 = width // 2
    per = BLOCK * planes

    def adjacent(lower, k):
        at = slice(k * width2, (k + 1) * width2)
        return pick(lower, even, from_a[at, :], from_b[at, :], first if lower else last)

    zs[2 : 4 + BLOCK] = zs_in[...]
    gs[2 : 2 + BLOCK] = gs_in[...]
    for k in range(2):
        spread_cell(adjacent(True, k).astype(F32), zs, k)
        spread_cell(adjacent(False, k).astype(F32), zs, 4 + BLOCK + k)
    pre = second_conv(zs, [1, 3 + BLOCK], 2, f2)
    slope = slope_of(pre, sigmoid(pre))
    for k in range(4):
        lower = k < 2
        cot = jnp.concatenate([adjacent(lower, 2 + 2 * g + k % 2) for g in range(2)], axis=1).astype(F32)
        spread_grad(cot * slope[k * width2 : (k + 1) * width2], gs, k if lower else BLOCK + k)

    inner = BLOCK + 2
    fields = jnp.concatenate([stacked(gs, [2 - t], inner) for t in range(3)], axis=1)
    back = mm(fields, b2[...].reshape(-1, wide1))
    pieces = wide1 // 128
    for u in range(inner):
        x = back[u * width2 : (u + 1) * width2]
        for piece in range(pieces):
            lanes = slice(piece * 128, (piece + 1) * 128)
            up[u * pieces + piece, pl.ds(0, width2, 2), :] = x[:, lanes]
            up[u * pieces + piece, pl.ds(1, width2, 2), :] = x[:, lanes]
    for u in range(per + 2):
        q = per - 1 + u
        both = [up[(q - 6) // 2 * pieces + piece] for piece in range(pieces)]
        if q <= per:
            slope = slopes_out[q - per + 2]
        elif q >= 2 * per - 1:
            slope = slopes_out[q - 2 * per + 4]
        else:
            slope = slopes_mid[q - per - 1]
        g = jnp.concatenate(both, axis=1) * slope
        if q < per:
            g = jnp.where(first, 0.0, g)
        if q >= 2 * per:
            g = jnp.where(last, 0.0, g)
        g1[u] = g.astype(BF16)

    center = g1[1 : 1 + per].reshape(per * width, wide1)
    parts = weight_product(center, xs, range(EDGE - 1, EDGE + 2), per)
    tiles = {}
    collect(d, parts, 1, d.height, d.mid, tiles, 0)
    for t, tile in tiles.items():
        late[t * d.mid : (t + 1) * d.mid, :] = tile.astype(BF16)
    grads_out[...] = g1[pl.ds((place & (BLOCK - 1)) * planes, planes + 2)]


def feats_grad(d, g1, b1, out, wide):
    planes, width, wide1 = d.planes, d.width, d.height * d.mid
    for u in range(planes + 2):
        g = g1[u]
        before, after = shifted(g.astype(F32))
        wide[u, :, 0:wide1] = after.astype(BF16)
        wide[u, :, wide1 : 2 * wide1] = g
        wide[u, :, 2 * wide1 :] = before.astype(BF16)
    fields = jnp.concatenate([stacked(wide, [2 - a], planes) for a in range(3)], axis=1)
    grad = mm(fields, b1[...].reshape(-1, d.height * d.half)).astype(BF16)
    grad = jnp.concatenate([grad[p * width : (p + 1) * width] for p in range(planes)], axis=1)
    turn = order_matrix(d.half, planes, d.height)
    out[...] = lax.dot_general(turn, grad, (((1,), (1,)), ((), ())), preferred_element_type=F32).astype(BF16)


def final_tiles(d, parts, groups):
    half, mid = d.half, d.mid
    slots = 128 // half
    for t in range(parts[0].shape[0] // mid):
        terms = [p[t * mid : (t + 1) * mid, :].astype(F32) for p in parts]
        while len(terms) > 1:
            terms = [terms[i] + terms[i + 1] for i in range(0, len(terms), 2)]
        tile = terms[0]
        if groups == 1:
            tile = pltpu.roll(tile, lax.axis_index("chan") * half, 0)
        flat = tile.T
        for slot in range(slots * t, min(slots * (t + 1), 27 * groups)):
            g, m, b = slot // 27, slot % 27 // 3, slot % 3
            spot = slot % slots
            yield g, 9 * (m // 3) + 3 * b + m % 3, flat[spot * half : (spot + 1) * half]


def fill_kernel(d, g1, b1, *refs):
    feats_out, out, wide, r = refs[-4:]
    feats_grad(d, g1, b1, feats_out, wide)
    member = lax.axis_index("chan")
    for g, tap, piece in final_tiles(d, refs[:-4], 2):
        r[g ^ member, tap * d.half : (tap + 1) * d.half, :] = piece
    out[...] = jnp.concatenate([r[0], r[1]], axis=1)


def final_kernel(d, *refs):
    out = refs[-1]
    for g, tap, piece in final_tiles(d, refs[:-1], 1):
        out[tap * d.half : (tap + 1) * d.half, :] = piece


class Sizes:
    pass


def shards(feats, weight_one, weight_two, cotangent):
    d = Sizes()
    slabs = lax.axis_size("depth")
    assert lax.axis_size("chan") == 2 and slabs % BLOCK == 0
    d.half, d.planes, d.height, d.width = feats.shape
    d.half2, coarse, d.height2, width2 = cotangent.shape
    d.mid = weight_one.shape[0]
    assert d.planes == 2 and coarse == 1 and d.half * 8 == 128 and d.height2 * d.half2 == 128
    assert d.width == 128 and d.height == 8 and d.mid == d.half2 == 32
    blocks = slabs // BLOCK
    per = BLOCK * d.planes
    wide1 = d.height * d.mid
    own1 = d.height * d.half
    wide2 = d.height2 * 2 * d.half2
    zl = d.height2 * d.mid

    def call(kernel, outs, scratch=(), flops=0, ins=None, mib=40, aliases=None):
        def run(*args):
            return pl.pallas_call(
                functools.partial(kernel, d),
                out_shape=[jax.ShapeDtypeStruct(shape, dtype) for shape, dtype in outs],
                in_specs=[pl.BlockSpec(memory_space=ins or pltpu.VMEM)] * len(args),
                out_specs=[VMEM] * len(outs),
                scratch_shapes=list(scratch),
                input_output_aliases=aliases or {},
                compiler_params=pltpu.CompilerParams(vmem_limit_bytes=mib << 20),
                cost_estimate=pl.CostEstimate(flops=flops, bytes_accessed=1 << 20, transcendentals=0),
            )(*args)

        return run

    rows = d.planes * d.width + width2
    feats_shape = (d.half * d.planes * d.height, d.width)
    cells = jnp.pad(cotangent.reshape(-1, width2), ((0, 0), (0, d.width - width2)))
    raw = jnp.concatenate([feats.reshape(feats_shape), cells])
    (item,) = call(pack_kernel, [((rows, 128), BF16)])(raw)

    def xor(x, k):
        return lax.ppermute(x, "depth", [(i, i ^ k) for i in range(slabs)])

    def gather(k):
        return xor(item, k)

    def swap(x):
        return lax.ppermute(x, "chan", [(0, 1), (1, 0)])

    side_rows = EDGE * d.width
    mid, to_a, to_b = call(
        sort_kernel, [((BLOCK * rows, 128), BF16), ((side_rows, 128), BF16), ((side_rows, 128), BF16)]
    )(item, *[gather(k) for k in range(1, BLOCK)])
    pair_a = [(i, i ^ BLOCK) for i in range(slabs)]
    inside = range(BLOCK, slabs - BLOCK)
    pair_b = [(i, ((i - BLOCK) ^ BLOCK) + BLOCK if i in inside else i) for i in range(slabs)]

    def trade(x_a, x_b):
        a = lax.ppermute(x_a, "depth", pair_a)
        b = lax.ppermute(x_b, "depth", pair_b)
        return a, b

    a, b = trade(to_a, to_b)
    mid_x, a_x, b_x = swap(mid), swap(a), swap(b)

    w1 = jnp.transpose(weight_one, (2, 0, 1)).reshape(27 * d.mid, d.mid)
    w2 = jnp.transpose(weight_two, (2, 1, 0)).reshape(27 * d.mid, 2 * d.half2)
    w1 = jnp.pad(w1, ((0, 0), (0, w2.shape[1] - w1.shape[1])))
    f1, b1, f2, b2 = call(
        weight_kernel,
        [
            ((3, 6 * own1, wide1), BF16),
            ((3, 3 * wide1, own1), BF16),
            ((3, 3 * zl, wide2), BF16),
            ((3, 3 * wide2, wide1), BF16),
        ],
        [
            pltpu.VMEM((27 * d.mid, wide1), BF16),
            pltpu.VMEM((27 * d.mid, own1), BF16),
            pltpu.VMEM((27 * d.mid, wide2), BF16),
            pltpu.VMEM((27 * 2 * d.half2, wide1), BF16),
        ],
        flops=1 << 30,
    )(jnp.concatenate([w1, w2]))
    xs_mid, xs_mid_x, slopes_mid, rows_mid, for_a, for_b = call(
        middle_kernel,
        [
            ((per + 2 * EDGE, d.width, 3 * own1), BF16),
            ((per + 2 * EDGE, d.width, 3 * own1), BF16),
            ((per - 2, d.width, wide1), F32),
            ((per - 2, d.width, zl), F32),
            ((6 * width2, zl), BF16),
            ((6 * width2, zl), BF16),
        ],
        [pltpu.VMEM((BLOCK - 2, d.width, zl), F32)],
        flops=1 << 30,
    )(mid, mid_x, f1)
    from_a, from_b = trade(for_a, for_b)
    ends_shape = (6 * d.width, wide1)
    xs, part = call(
        outer_kernel, [((per + 2 * EDGE, d.width, 3 * own1), BF16), (ends_shape, F32)], flops=1 << 30, aliases={2: 0}
    )(a, b, xs_mid, f1)
    _, slopes_out, rows_out = call(
        close_kernel,
        [
            ((per + 2 * EDGE, d.width, 3 * own1), BF16),
            ((6, d.width, wide1), F32),
            ((6, d.width, zl), F32),
        ],
        flops=1 << 30,
        aliases={2: 0},
    )(a_x, b_x, xs_mid_x, f1, part)

    def gather_sums(x):
        radix = 1
        parts = [x]
        while radix < blocks:
            x = sum_parts(parts)
            fan = min(4, blocks // radix)
            parts = [None] * fan
            for k in range(fan - 1, 0, -1):
                parts[k] = xor(x, BLOCK * radix * k)
            parts[0] = x
            radix *= fan
        return parts

    early_rows, late_rows = -(-2 * 27 // 8) * d.half2, -(-27 // 8) * d.mid
    zs, gs, early = call(
        second_kernel,
        [
            ((BLOCK + 2, width2, 3 * zl), BF16),
            ((BLOCK, width2, 3 * wide2), BF16),
            ((early_rows, 128), BF16),
        ],
        [pltpu.VMEM((BLOCK, d.width, zl), F32)],
        flops=1 << 30,
    )(mid, mid_x, for_a, rows_mid, rows_out, f2)
    early = gather_sums(early)
    grads, late = call(
        main_kernel,
        [
            ((d.planes + 2, d.width, wide1), BF16),
            ((late_rows, 128), BF16),
        ],
        [
            pltpu.VMEM((3 * BLOCK - 2, width2, 3 * zl), BF16),
            pltpu.VMEM((BLOCK + 4, width2, 3 * wide2), BF16),
            pltpu.VMEM(((BLOCK + 2) * (wide1 // 128), d.width, 128), F32),
            pltpu.VMEM((per + 2, d.width, wide1), BF16),
        ],
        flops=1 << 32,
    )(xs, slopes_mid, slopes_out, from_a, from_b, zs, gs, f2, b2)

    late = gather_sums(late)
    grad, out2 = call(
        fill_kernel,
        [(feats_shape, BF16), ((27 * d.half, 2 * d.half2), F32)],
        [
            pltpu.VMEM((d.planes + 2, d.width, 3 * wide1), BF16),
            pltpu.VMEM((2, 27 * d.half, d.mid), F32),
        ],
        flops=1 << 30,
    )(grads, b1, *early)
    (out1,) = call(final_kernel, [((27 * d.half, d.mid), F32)])(*late)
    return (
        grad.reshape(feats.shape),
        out1.reshape(27, d.half, d.mid).transpose(2, 1, 0),
        out2.reshape(27, d.half, 2 * d.half2).transpose(2, 1, 0),
    )


def sum_parts(parts):
    if len(parts) == 1:
        return parts[0]
    terms = [p.astype(F32) for p in parts]
    while len(terms) > 1:
        terms = [terms[i] + terms[i + 1] for i in range(0, len(terms), 2)]
    return terms[0].astype(BF16)


def solution(mesh):
    return jax.shard_map(
        shards,
        mesh=mesh,
        in_specs=(P("chan", "depth", None, None), P(), P(), P("chan", "depth", None, None)),
        out_specs=(P("chan", "depth", None, None), P(None, "chan", None), P(None, "chan", None)),
        check_vma=False,
    )
```
